128 devices in a mesh: gx: 16 (over y, x), gy: 4 (over z), gz: 2 (over core).
Axes of the slice: x: 4, y: 4, z: 4, core: 2. Of those that a mesh axis runs over, the one named last changes fastest.
Arguments:
- load: float32 [1024, 256, 256], P('gx', 'gy', 'gz'), may hold values from -12 to 12
- stiffness: float32 [1024, 256, 256], P('gx', 'gy', 'gz'), may hold values from 0.02 to 2
- prestress: float32 [1024, 256], P(('gx', 'gy'), 'gz'), may hold values from -3 to 3
- state_var: float32 [1024, 256], P(('gx', 'gy'), 'gz'), may hold values from -1 to 1
- normal_a: float32 [1024, 256], P(('gx', 'gy'), 'gz'), may hold values from 1 to 3
Outputs:
- displacement: float32 [1024, 256, 256], P('gx', 'gy', 'gz')
- slip_rate: float32 [1024, 256], P(('gx', 'gy'), 'gz')
The draws below stay inside these ranges and needn't reach their ends.
All inputs are finite; a program needn't handle non-finite values.
Results may differ from the reference program's by a relative error of at most 0.0003.
Values sent between devices are 32-bit elements; how exact they have to be, the bound alone decides.
No kernel may reach another device: no remote copies, remote signals or barrier semaphores. Data moves between devices by JAX's collectives and lax.ppermute only.
A program may use at most 128 MiB of HBM per device.

```python
import math
import jax
import jax.numpy as jnp

ITERS = 3
NX = 1024
NY = 256
NZ = 256


def draw_load(key, part):
    subkeys = jax.random.split(key, 4)
    along_x = ((jnp.arange(NX, dtype=jnp.float32) + 0.5) / NX)[:, None, None]
    along_y = ((jnp.arange(NY, dtype=jnp.float32) + 0.5) / NY)[None, :, None]
    along_z = ((jnp.arange(NZ, dtype=jnp.float32) + 0.5) / NZ)[None, None, :]
    waves_x = jax.random.randint(subkeys[0], (4,), 1, 4).astype(jnp.float32)
    waves_z = jax.random.randint(subkeys[1], (4,), 0, 2).astype(jnp.float32)
    phases = jax.random.uniform(subkeys[2], (7,), jnp.float32, 0.0, 2.0 * math.pi)
    smooth = jnp.zeros((NX, NY, NZ), jnp.float32)
    for mode_num in range(4):
        smooth = smooth + jnp.cos(2.0 * math.pi * (waves_x[mode_num] * along_x + along_y + waves_z[mode_num] * along_z) + phases[mode_num])
    smooth = smooth * 0.7071
    exponent = 0.5 + 0.25 * jnp.sin(2.0 * math.pi * along_x + phases[4]) + 0.25 * jnp.sin(2.0 * math.pi * along_y + phases[5])
    rough_scale = 0.3 * jnp.exp(exponent * math.log(5.0))
    smooth_scale = 0.4 + 0.4 * (1.0 + jnp.cos(2.0 * math.pi * along_z + phases[6]))
    white_noise = jax.random.truncated_normal(subkeys[3], -4.0, 4.0, (NX, NY, NZ), jnp.float32)
    return (smooth_scale * smooth + rough_scale * white_noise).astype(jnp.float32)


def level_of(rng, shape, cuts, smallest, top_value):
    factor_of = 1.0
    for dim, blocks in cuts:
        steps = jax.random.uniform(jax.random.fold_in(jax.random.fold_in(rng, 6), dim), (blocks,), jnp.float32, smallest / len(cuts), top_value / len(cuts))
        factor_of = factor_of * jnp.repeat(jnp.exp(steps), shape[dim] // blocks).reshape((-1,) + (1,) * (len(shape) - 1 - dim))
    return factor_of


def bell_draw(key, shape, spread, limit, cuts=(), kind=jnp.bfloat16):
    result = spread * jax.random.normal(key, shape, jnp.float32)
    if cuts:
        result = result * level_of(key, shape, cuts, -0.22, 0.18)
    return jnp.clip(result, -limit, limit).astype(kind)


def setup_inputs(seed: int = 0) -> dict:
    key_list = jax.random.split(jax.random.key(seed), 6)
    return {
        "load": draw_load(jax.random.fold_in(key_list[5], 71), 0),
        "stiffness": jnp.clip(jnp.exp(math.log(2.0) - 4.6051702 * jax.random.uniform(key_list[1], (NX, NY, NZ), jnp.float32) ** level_of(key_list[1], (NX, NY, NZ), ((0, 16), (1, 4), (2, 2)), -0.2, 0.2)), 0.02, 2.0),
        "prestress": bell_draw(key_list[2], (NX, NZ), 1.0, 3.0, ((0, 64), (1, 2)), jnp.float32),
        "state_var": jnp.clip(jax.random.uniform(key_list[3], (NX, NZ), jnp.float32, -1.0, 1.0) * level_of(key_list[3], (NX, NZ), ((0, 64), (1, 2)), -0.4, 0.0), -1.0, 1.0),
        "normal_a": jnp.clip(jnp.exp(math.log(3.0) - 1.0986123 * jax.random.uniform(key_list[4], (NX, NZ), jnp.float32) ** level_of(key_list[4], (NX, NZ), ((0, 64), (1, 2)), -0.2, 0.2)), 1.0, 3.0),
    }


def shifted(padded, sizes_now, axis_num, offset):
    slicers = [slice(2, 2 + sizes_now[0]), slice(2, 2 + sizes_now[1]), slice(2, 2 + sizes_now[2])]
    slicers[axis_num] = slice(2 + offset, 2 + offset + sizes_now[axis_num])
    return padded[tuple(slicers)]


def operate(field, stiffness):
    padded = jnp.pad(field, 2)
    sizes_now = field.shape
    near_sum = jnp.zeros_like(field)
    for axis_num in range(3):
        near_sum = near_sum + 16.0 * (shifted(padded, sizes_now, axis_num, 1) + shifted(padded, sizes_now, axis_num, -1))
        near_sum = near_sum - (shifted(padded, sizes_now, axis_num, 2) + shifted(padded, sizes_now, axis_num, -2))
    return (7.5 + stiffness) * field - near_sum / 12.0


def reference(load, stiffness, prestress, state_var, normal_a):
    inverse = 1.0 / (7.5 + stiffness)
    solution = jnp.zeros_like(load)
    residual = load
    precond = inverse * residual
    direction = precond
    gamma = jnp.sum(residual * precond)
    for iteration in range(ITERS):
        image = operate(direction, stiffness)
        alpha = gamma / jnp.sum(direction * image)
        solution = solution + alpha * direction
        residual = residual - alpha * image
        if iteration + 1 < ITERS:
            precond = inverse * residual
            gamma_new = jnp.sum(residual * precond)
            direction = precond + (gamma_new / gamma) * direction
            gamma = gamma_new
    half = NY // 2
    traction = (solution[:, half - 2, :] - 27.0 * solution[:, half - 1, :]
                + 27.0 * solution[:, half, :] - solution[:, half + 1, :]) / 24.0
    slip_rate = jnp.exp(-state_var) * jnp.sinh((prestress + 2.0 * traction) / normal_a)
    return solution, slip_rate
```

```python
import functools

import jax
import jax.numpy as jnp
from jax import lax
from jax.experimental import pallas as pl
from jax.experimental.pallas import tpu as pltpu
from jax.sharding import Mesh
from jax.sharding import PartitionSpec as P

GX = ("gx_0", "gx_1")
GX_GY = ("gx_0", "gx_1", "gy")
ALL = ("gx_0", "gx_1", "gy", "gz")
F32 = jnp.float32

NXL, NYL, NZL = 64, 64, 128
PX, PY = NXL + 4, NYL + 16
Y0 = 8


def vmem(shape):
    return pltpu.VMEM(shape, F32)


def in_vmem(x):
    return pltpu.with_memory_space_constraint(x, pltpu.VMEM)


def place():
    gx = lax.axis_index("gx_0") * lax.axis_size("gx_1") + lax.axis_index("gx_1")
    return gx, lax.axis_index("gy"), lax.axis_index("gz")


def lanes():
    return lax.broadcasted_iota(jnp.int32, (NYL, NZL), 1)


def fold(x):
    return x.reshape(NYL // 8, 8, NZL).sum(axis=0)


def pack_z(x, plane, packed, gz):
    lane = lanes()
    shift = lax.rem(2 * x + 2 * (1 - gz), NZL)
    return jnp.where(lane // 2 == x, pltpu.roll(plane, shift, 1), packed)


def send_faces(kp, ex, ox, ey, oy):
    gx, gy, _ = place()
    even = lax.rem(gx, 2) == 0

    @pl.when(even)
    def _():
        ex[...] = kp[NXL : NXL + 2, Y0 : Y0 + NYL, :]
        ox[...] = kp[2:4, Y0 : Y0 + NYL, :]

    @pl.when(jnp.logical_not(even))
    def _():
        ox[...] = kp[NXL : NXL + 2, Y0 : Y0 + NYL, :]
        ex[...] = kp[2:4, Y0 : Y0 + NYL, :]

    def rows(up, down):
        for x in range(NXL):
            for k in range(2):
                up[k, x : x + 1, :] = kp[x + 2, Y0 + NYL - 2 + k : Y0 + NYL - 1 + k, :]
                down[k, x : x + 1, :] = kp[x + 2, Y0 + k : Y0 + 1 + k, :]

    even_y = lax.rem(gy, 2) == 0

    @pl.when(even_y)
    def _():
        rows(ey, oy)

    @pl.when(jnp.logical_not(even_y))
    def _():
        rows(oy, ey)


def take_faces(kp, exr, oxr, eyr, oyr):
    gx, gy, _ = place()
    inner = jnp.logical_and(gx != 0, gx != 15)
    even = lax.rem(gx, 2) == 0

    @pl.when(even)
    def _():
        kp[NXL + 2 : NXL + 4, Y0 : Y0 + NYL, :] = exr[...]
        kp[0:2, Y0 : Y0 + NYL, :] = jnp.where(inner, oxr[...], 0.0)

    @pl.when(jnp.logical_not(even))
    def _():
        kp[NXL + 2 : NXL + 4, Y0 : Y0 + NYL, :] = jnp.where(inner, oxr[...], 0.0)
        kp[0:2, Y0 : Y0 + NYL, :] = exr[...]

    inner_y = jnp.logical_and(gy != 0, gy != 3)
    even_y = lax.rem(gy, 2) == 0

    def rows(up, down, up_masked):
        for x in range(NXL):
            for k in range(2):
                high = up[k, x : x + 1, :]
                low = down[k, x : x + 1, :]
                if up_masked:
                    high = jnp.where(inner_y, high, 0.0)
                else:
                    low = jnp.where(inner_y, low, 0.0)
                kp[x + 2, Y0 + NYL + k : Y0 + NYL + 1 + k, :] = high
                kp[x + 2, Y0 - 2 + k : Y0 - 1 + k, :] = low

    @pl.when(even_y)
    def _():
        rows(eyr, oyr, False)

    @pl.when(jnp.logical_not(even_y))
    def _():
        rows(oyr, eyr, True)


def z_terms(zr):
    gz = lax.axis_index("gz")
    lane = lanes()
    got = zr[...]
    odd = lax.rem(lane, 2) == 1
    low = jnp.where(odd, pltpu.roll(got, 1, 1), 0.0)
    high = jnp.where(odd, 0.0, pltpu.roll(got, NZL - 1, 1))
    return 16.0 * jnp.where(gz == 0, low, high) - got


def stencil(kp, x, terms, gz):
    lane = lanes()
    own = slice(Y0, Y0 + NYL)
    here = kp[x + 2, own, :]
    near = kp[x + 1, own, :] + kp[x + 3, own, :]
    far = kp[x, own, :] + kp[x + 4, own, :]
    near = near + (kp[x + 2, Y0 - 1 : Y0 + NYL - 1, :] + kp[x + 2, Y0 + 1 : Y0 + NYL + 1, :])
    far = far + (kp[x + 2, Y0 - 2 : Y0 + NYL - 2, :] + kp[x + 2, Y0 + 2 : Y0 + NYL + 2, :])
    near = near + jnp.where(lane >= 1, pltpu.roll(here, 1, 1), 0.0)
    near = near + jnp.where(lane < NZL - 1, pltpu.roll(here, NZL - 1, 1), 0.0)
    far = far + jnp.where(lane >= 2, pltpu.roll(here, 2, 1), 0.0)
    far = far + jnp.where(lane < NZL - 2, pltpu.roll(here, NZL - 2, 1), 0.0)
    side = lane // 2 == (NZL // 2 - 1) * (1 - gz)
    shift = lax.rem(NZL - 2 * x + (NZL - 2) * (1 - gz), NZL)
    far = far - jnp.where(side, pltpu.roll(terms, shift, 1), 0.0)
    return here, (16.0 * near - far) * (1.0 / 12.0)


def first_kernel(load, stiff, b, dinv, kp, ex, ox, ey, oy, z, sums, s, sem_b, sem_s):
    parts = 4
    step = NXL // parts
    gz = lax.axis_index("gz")

    def copies(i):
        at = pl.ds(i * step, step)
        return (
            pltpu.make_async_copy(load.at[at], b.at[at], sem_b.at[i]),
            pltpu.make_async_copy(stiff.at[at], s.at[at], sem_s.at[i]),
        )

    for i in range(parts):
        for c in copies(i):
            c.start()

    def plane(x, carry):
        packed, total = carry
        inverse = 1.0 / (7.5 + s[x])
        right = b[x]
        k = right * inverse
        dinv[x] = inverse
        kp[x + 2, Y0 : Y0 + NYL, :] = k
        return pack_z(x, k, packed, gz), total + fold(k * right)

    carry = (jnp.zeros((NYL, NZL), F32), jnp.zeros((8, NZL), F32))
    for i in range(parts):
        for c in copies(i):
            c.wait()
        carry = lax.fori_loop(i * step, (i + 1) * step, plane, carry)
    z[...] = carry[0]
    sums[0] = carry[1]
    send_faces(kp, ex, ox, ey, oy)


def stage_kernel(
    first, kp_in, exr, oxr, eyr, oyr, zr, prev, dinv, kp, kn, acc, ex, ox, ey, oy, z, sums
):
    del kp_in
    gz = lax.axis_index("gz")
    take_faces(kp, exr, oxr, eyr, oyr)
    terms = z_terms(zr)

    def plane(x, carry):
        packed, s0, s1, s2 = carry
        here, a = stencil(kp, x, terms, gz)
        k = a * dinv[x]
        acc[x] = a
        kn[x + 2, Y0 : Y0 + NYL, :] = k
        before = prev[x]
        change = before - a
        s0 = s0 + fold(here * change)
        s1 = s1 + fold(k * change)
        s2 = s2 + fold((k if first else here) * before)
        return pack_z(x, k, packed, gz), s0, s1, s2

    zero = jnp.zeros((8, NZL), F32)
    packed, s0, s1, s2 = lax.fori_loop(0, NXL, plane, (jnp.zeros((NYL, NZL), F32), zero, zero, zero))
    z[...] = packed
    sums[0] = s0
    sums[1] = s1
    sums[2] = s2
    send_faces(kn, ex, ox, ey, oy)


def last_kernel(kp_in, k0, k1, exr, oxr, eyr, oyr, zr, prev, sums0, sums1, sums2, kp, row, own, sent, t):
    del kp_in
    _, gy, gz = place()
    take_faces(kp, exr, oxr, eyr, oyr)
    terms = z_terms(zr)

    def plane(x, total):
        here, a = stencil(kp, x, terms, gz)
        return total + fold(here * (prev[x] - a))

    m4 = lax.fori_loop(0, NXL, plane, jnp.zeros((8, NZL), F32))
    parts = (
        sums0[0], sums1[2], sums2[2], sums1[0], sums1[1], sums2[0], sums2[1], m4,
    )
    lane = lax.broadcasted_iota(jnp.int32, (1, NZL), 1)
    out = jnp.zeros((1, NZL), F32)
    for i, part in enumerate(parts):
        out = jnp.where(lane == i, jnp.sum(jnp.sum(part, axis=0, keepdims=True), axis=1, keepdims=True), out)
    row[...] = jnp.broadcast_to(out, (128, NZL))

    def traction(base):
        for j, ref in enumerate((k0, k1, kp)):
            for x in range(NXL):
                r = [ref[x + 2, base + i : base + i + 1, :] for i in range(4)]
                t[j, x : x + 1, :] = (r[0] - r[3] + 27.0 * (r[2] - r[1])) * (1.0 / 24.0)

    @pl.when(gy == 1)
    def _():
        traction(Y0 + NYL - 2)
        sent[...] = t[:, 0:16, :]
        own[...] = t[:, 16:32, :]

    @pl.when(gy == 2)
    def _():
        traction(Y0 - 2)
        sent[...] = t[:, 48:64, :]
        own[...] = t[:, 32:48, :]

    @pl.when(jnp.logical_or(gy == 0, gy == 3))
    def _():
        sent[...] = jnp.zeros_like(sent)
        own[...] = jnp.zeros_like(own)


def coefficients(rows):
    tot = jnp.sum(rows, axis=0, keepdims=True)
    lane = lax.broadcasted_iota(jnp.int32, (1, NZL), 1)
    v = [jnp.sum(jnp.where(lane == i, tot, 0.0), axis=1, keepdims=True) for i in range(8)]
    v0, v1, v2, m0, m1, m2, m3, m4 = v
    l1 = m1 / m0
    l2 = m2 / m0
    d1 = m2 - l1 * m1
    e = m3 - l2 * m1
    f1 = v1 - l1 * v0
    l3 = e / d1
    d2 = (m4 - l2 * m2) - l3 * e
    f2 = (v2 - l2 * v0) - l3 * f1
    c2 = f2 / d2
    c1 = (f1 - e * c2) / d1
    c0 = (v0 - m1 * c1 - m2 * c2) / m0
    return c0, c1, c2


def scaled_sinh(a, s):
    half = 0.6931471805599453
    large = jnp.exp(a - s - half) - jnp.exp(-a - s - half)
    q = a * a
    small = a * (1.0 + q * (1.0 / 6.0 + q * (1.0 / 120.0 + q * (1.0 / 5040.0)))) * jnp.exp(-s)
    return jnp.where(jnp.abs(a) < 0.5, small, large)


def final_kernel(k0, k1, k2, rows, own, got, prestress, state, normal, out, slip, buf, sem):
    gy = lax.axis_index("gy")
    parts = 4
    step = NXL // parts
    c0, c1, c2 = coefficients(rows[...])

    def copy(i):
        at = pl.ds(i * step, step)
        return pltpu.make_async_copy(buf.at[at], out.at[at], sem.at[i])

    def plane(x, carry):
        at = slice(Y0, Y0 + NYL)
        buf[x] = c0 * k0[x + 2, at, :] + c1 * k1[x + 2, at, :] + c2 * k2[x + 2, at, :]
        return carry

    for i in range(parts):
        lax.fori_loop(i * step, (i + 1) * step, plane, 0)
        copy(i).start()
    mine = jnp.logical_or(gy == 1, gy == 2)
    t = jnp.where(mine, own[...], got[...])
    traction = c0 * t[0] + c1 * t[1] + c2 * t[2]
    arg = (prestress[...] + 2.0 * traction) / normal[...]
    slip[...] = scaled_sinh(arg, state[...])
    for i in range(parts):
        copy(i).wait()


def swap(x, axes, pairs):
    return lax.ppermute(x, axes, [*pairs, *((b, a) for a, b in pairs)])


def exchange(ex, ox, ey, oy, z):
    evens = [(2 * i, 2 * i + 1) for i in range(8)]
    odds = [(2 * i + 1, (2 * i + 2) % 16) for i in range(8)]
    return (
        swap(ex, GX, evens),
        swap(ox, GX, odds),
        swap(ey, "gy", [(0, 1), (2, 3)]),
        swap(oy, "gy", [(1, 2), (3, 0)]),
        swap(z, "gz", [(0, 1)]),
    )


VM = pl.BlockSpec(memory_space=pltpu.VMEM)
HB = pl.BlockSpec(memory_space=pl.ANY)
FACE = (2, NYL, NZL)
FACES = (FACE, (2, NYL, NZL), (2, NXL, NZL), (2, NXL, NZL), (NYL, NZL))
BLOCK = (NXL, NYL, NZL)
PADDED = (PX, PY, NZL)


def params():
    return pltpu.CompilerParams(vmem_limit_bytes=24 * 2**20)


def cost(flops, nbytes):
    return pl.CostEstimate(flops=flops, bytes_accessed=nbytes, transcendentals=0)


def stage(first, kp, faces, prev, dinv):
    outs = (PADDED, PADDED, BLOCK, *FACES, (3, 8, NZL))
    return pl.pallas_call(
        functools.partial(stage_kernel, first),
        out_shape=tuple(vmem(s) for s in outs),
        in_specs=[VM] * 8,
        out_specs=(VM,) * len(outs),
        input_output_aliases={0: 0},
        compiler_params=params(),
        cost_estimate=cost(20_000_000, 10_000_000),
        name="stage_one" if first else "stage_two",
    )(*map(in_vmem, (kp, *faces, prev, dinv)))


def per_device(load, stiffness, prestress, state_var, normal_a):
    outs = (BLOCK, BLOCK, PADDED, *FACES, (1, 8, NZL))
    b, dinv, k0, *rest = pl.pallas_call(
        first_kernel,
        out_shape=tuple(vmem(s) for s in outs),
        in_specs=[HB, HB],
        out_specs=(VM,) * len(outs),
        scratch_shapes=[vmem(BLOCK), pltpu.SemaphoreType.DMA((4,)), pltpu.SemaphoreType.DMA((4,))],
        compiler_params=params(),
        cost_estimate=cost(20_000_000, 10_000_000),
        name="start",
    )(load, stiffness)
    sums0 = rest[-1]
    k0, k1, acc0, *rest = stage(True, k0, exchange(*rest[:-1]), b, dinv)
    sums1 = rest[-1]
    k1, k2, acc1, *rest = stage(False, k1, exchange(*rest[:-1]), acc0, dinv)
    sums2 = rest[-1]
    faces = exchange(*rest[:-1])
    outs = (PADDED, (128, NZL), (3, 16, NZL), (3, 16, NZL))
    k2, row, own, sent = pl.pallas_call(
        last_kernel,
        out_shape=tuple(vmem(s) for s in outs),
        in_specs=[VM] * 12,
        out_specs=(VM,) * len(outs),
        input_output_aliases={0: 0},
        scratch_shapes=[vmem((3, NXL, NZL))],
        compiler_params=params(),
        cost_estimate=cost(20_000_000, 10_000_000),
        name="last",
    )(*map(in_vmem, (k2, k0, k1, *faces, acc1, sums0, sums1, sums2)))
    got = swap(sent, "gy", [(0, 1), (2, 3)])
    rows = lax.all_to_all(row, ALL, 0, 0, tiled=True)
    out, slip = pl.pallas_call(
        final_kernel,
        out_shape=(jax.ShapeDtypeStruct(BLOCK, F32), jax.ShapeDtypeStruct((16, NZL), F32)),
        in_specs=[VM] * 9,
        out_specs=(HB, VM),
        scratch_shapes=[vmem(BLOCK), pltpu.SemaphoreType.DMA((4,))],
        compiler_params=params(),
        cost_estimate=cost(20_000_000, 10_000_000),
        name="final",
    )(*map(in_vmem, (k0, k1, k2, rows, own, got)), prestress, state_var, normal_a)
    return out, slip


def solution(mesh):
    torus = Mesh(
        mesh.devices.reshape(4, 4, mesh.shape["gy"], mesh.shape["gz"]), ("gx_0", "gx_1", "gy", "gz")
    )
    block = P(GX, "gy", "gz")
    fault = P(GX_GY, "gz")
    return jax.shard_map(
        per_device,
        mesh=torus,
        in_specs=(block, block, fault, fault, fault),
        out_specs=(block, fault),
        check_vma=False,
    )
```

```python
import functools

import jax
import jax.numpy as jnp
from jax import lax
from jax.experimental import pallas as pl
from jax.experimental.pallas import tpu as pltpu
from jax.sharding import Mesh
from jax.sharding import PartitionSpec as P

GX = ("gx_0", "gx_1")
GX_GY = ("gx_0", "gx_1", "gy")
ALL = ("gx_0", "gx_1", "gy", "gz")
F32 = jnp.float32

NXL, NYL, NZL = 64, 64, 128
PX = NXL + 4
PARTS = 8
TILES = 8
LIMIT = 6 * 2**20


def vmem(shape):
    return pltpu.VMEM(shape, F32)


def in_vmem(x):
    return pltpu.with_memory_space_constraint(x, pltpu.VMEM)


def place():
    gx = lax.axis_index("gx_0") * lax.axis_size("gx_1") + lax.axis_index("gx_1")
    return gx, lax.axis_index("gy"), lax.axis_index("gz")


def lanes():
    return lax.broadcasted_iota(jnp.int32, (8, NZL), 1)


def pack_z(x, tile, packed):
    shift = lax.rem(4 * x + 2 + NZL, NZL)
    return jnp.where(lanes() // 4 == lax.rem(x, 32), pltpu.roll(tile, shift, 1), packed)


def finish_plane(kn, x, packed):
    tiles = [kn[x + 2, v + 2] for v in range(TILES)]
    kn[x + 2, 0] = pltpu.roll(tiles[6], 1, 0)
    kn[x + 2, 1] = pltpu.roll(tiles[7], 1, 0)
    kn[x + 2, 10] = pltpu.roll(tiles[0], 7, 0)
    kn[x + 2, 11] = pltpu.roll(tiles[1], 7, 0)
    return tuple(pack_z(x, t, p) for t, p in zip(tiles, packed))


def zeros(n):
    return tuple(jnp.zeros((8, NZL), F32) for _ in range(n))


def send_faces(kp, ex, ox, ey, oy):
    gx, gy, _ = place()
    even = lax.rem(gx, 2) == 0

    def planes(up, down):
        up[...] = kp[NXL : NXL + 2, 2:10]
        down[...] = kp[2:4, 2:10]

    @pl.when(even)
    def _():
        planes(ex, ox)

    @pl.when(jnp.logical_not(even))
    def _():
        planes(ox, ex)

    def rows(up, down):
        for x in range(NXL):
            for k in range(2):
                up[k, x : x + 1, :] = kp[x + 2, 8 + k, 7:8, :]
                down[k, x : x + 1, :] = kp[x + 2, 2 + k, 0:1, :]

    even_y = lax.rem(gy, 2) == 0

    @pl.when(even_y)
    def _():
        rows(ey, oy)

    @pl.when(jnp.logical_not(even_y))
    def _():
        rows(oy, ey)


def take_faces(kp, exr, oxr, eyr, oyr):
    gx, gy, _ = place()
    inner = jnp.logical_and(gx != 0, gx != 15)
    even = lax.rem(gx, 2) == 0

    @pl.when(even)
    def _():
        kp[NXL + 2 : NXL + 4, 2:10] = exr[...]
        kp[0:2, 2:10] = jnp.where(inner, oxr[...], 0.0)

    @pl.when(jnp.logical_not(even))
    def _():
        kp[NXL + 2 : NXL + 4, 2:10] = jnp.where(inner, oxr[...], 0.0)
        kp[0:2, 2:10] = exr[...]

    inner_y = jnp.logical_and(gy != 0, gy != 3)
    even_y = lax.rem(gy, 2) == 0

    def rows(up, down, up_masked):
        for x in range(NXL):
            for k in range(2):
                high = up[k, x : x + 1, :]
                low = down[k, x : x + 1, :]
                if up_masked:
                    high = jnp.where(inner_y, high, 0.0)
                else:
                    low = jnp.where(inner_y, low, 0.0)
                kp[x + 2, 10 + k, 7:8, :] = high
                kp[x + 2, k, 0:1, :] = low

    @pl.when(even_y)
    def _():
        rows(eyr, oyr, False)

    @pl.when(jnp.logical_not(even_y))
    def _():
        rows(oyr, eyr, True)


def z_terms(terms, z, zr):
    gz = lax.axis_index("gz")
    at = lax.rem(lanes(), 4)
    ours = (at >= 2) == (gz == 0)
    for h in range(2):
        for v in range(TILES):
            d = jnp.where(ours, zr[h, v], 0.0) - z[h, v]
            two = jnp.where(at < 2, pltpu.roll(d, NZL - 2, 1), pltpu.roll(d, 2, 1))
            one = jnp.where(at == 1, pltpu.roll(d, NZL - 1, 1), jnp.where(at == 2, pltpu.roll(d, 1, 1), 0.0))
            terms[h, v] = 16.0 * one - two


def z_part(kp, x, half, terms, zbuf):
    lane = lanes()
    shift = lax.rem(126 + 2 * NZL - 4 * x, NZL)
    edge = jnp.logical_or(lane < 2, lane >= NZL - 2)
    for v in range(TILES):
        here = kp[x + 2, v + 2]
        near = pltpu.roll(here, 1, 1) + pltpu.roll(here, NZL - 1, 1)
        far = pltpu.roll(here, 2, 1) + pltpu.roll(here, NZL - 2, 1)
        zbuf[x, v] = (16.0 * near - far) + jnp.where(edge, pltpu.roll(terms[half, v], shift, 1), 0.0)


def stencil(kp, x, zbuf):
    p = [kp[x + 2, j] for j in range(TILES + 4)]
    for v in range(TILES):
        near = (kp[x + 1, v + 2] + kp[x + 3, v + 2]) + (p[v + 1] + p[v + 3])
        far = (kp[x, v + 2] + kp[x + 4, v + 2]) + (p[v] + p[v + 4])
        yield v, p[v + 2], (16.0 * near - far) + zbuf[x, v]


def first_kernel(load, stiff, b, dinv, kp, ex, ox, ey, oy, z, sums, raw, s, sem_b, sem_s):
    step = NXL // PARTS

    def copies(i):
        at = pl.ds(i * step, step)
        return (
            pltpu.make_async_copy(load.at[at], raw.at[at], sem_b.at[i]),
            pltpu.make_async_copy(stiff.at[at], s.at[at], sem_s.at[i]),
        )

    for i in range(PARTS):
        for c in copies(i):
            c.start()

    def planes(i, carry):
        packed, total = carry
        for x in (2 * i - 2, 2 * i - 1):
            packed = finish_plane(kp, x, packed)
        for x in (2 * i, 2 * i + 1):
            for v in range(TILES):
                row = pl.ds(v, 8, stride=TILES)
                inverse = 1.0 / (90.0 + 12.0 * s[x, row, :])
                right = 12.0 * raw[x, row, :]
                k = right * inverse
                b[x, v] = right
                dinv[x, v] = inverse
                kp[x + 2, v + 2] = k
                total = total + k * right
        return packed, total

    (total,) = zeros(1)
    packed = zeros(TILES)
    for i in range(PARTS):
        for c in copies(i):
            c.wait()
        if i == 0:
            kp[0:2, 2:10] = jnp.zeros((2, TILES, 8, NZL), F32)
        packed, total = lax.fori_loop(i * step // 2, (i + 1) * step // 2, planes, (packed, total))
        if (i + 1) * step % 32 == 0:
            for x in ((i + 1) * step - 2, (i + 1) * step - 1):
                packed = finish_plane(kp, x, packed)
            for v in range(TILES):
                z[(i + 1) * step // 32 - 1, v] = packed[v]
    sums[0] = total
    send_faces(kp, ex, ox, ey, oy)


def stage_kernel(
    kp_in, exr, oxr, eyr, oyr, zr, zo, prev, dinv, kp, kn, acc, ex, ox, ey, oy, z, sums, terms, zbuf
):
    del kp_in
    take_faces(kp, exr, oxr, eyr, oyr)
    z_terms(terms, zo, zr)
    for x in range(2):
        z_part(kp, x, 0, terms, zbuf)
    kn[0:2, 2:10] = jnp.zeros((2, TILES, 8, NZL), F32)

    def planes(i, carry, half):
        packed, s0, s1 = carry
        for x in (2 * i - 2, 2 * i - 1):
            packed = finish_plane(kn, x, packed)
        for x in (2 * i, 2 * i + 1):
            for v, here, a in stencil(kp, x, zbuf):
                change = prev[x, v] - a
                k = change * dinv[x, v]
                acc[x, v] = change
                kn[x + 2, v + 2] = k
                s0 = s0 + here * change
                s1 = s1 + k * change
        for x in (2 * i + 2, 2 * i + 3):
            z_part(kp, x, half, terms, zbuf)
        return packed, s0, s1

    carry = (zeros(TILES), *zeros(2))
    for h in range(2):
        carry = lax.fori_loop(16 * h, 16 * h + 15, functools.partial(planes, half=h), carry)
        packed, s0, s1 = planes(16 * h + 15, carry, 1)
        for x in (32 * h + 30, 32 * h + 31):
            packed = finish_plane(kn, x, packed)
        for v in range(TILES):
            z[h, v] = packed[v]
        carry = (packed, s0, s1)
    sums[0] = s0
    sums[1] = s1
    send_faces(kn, ex, ox, ey, oy)


def last_kernel(
    kp_in, k0, k1, exr, oxr, eyr, oyr, zr, zo, prev, sums0, sums1, sums2, kp, row, own, sent, t, terms, zbuf
):
    del kp_in
    gy = lax.axis_index("gy")
    take_faces(kp, exr, oxr, eyr, oyr)
    z_terms(terms, zo, zr)
    for x in range(2):
        z_part(kp, x, 0, terms, zbuf)

    def planes(i, total, half):
        for x in (2 * i, 2 * i + 1):
            for v, here, a in stencil(kp, x, zbuf):
                total = total + here * (prev[x, v] - a)
        for x in (2 * i + 2, 2 * i + 3):
            z_part(kp, x, half, terms, zbuf)
        return total

    (m4,) = zeros(1)
    for h in range(2):
        m4 = lax.fori_loop(16 * h, 16 * h + 15, functools.partial(planes, half=h), m4)
        m4 = planes(16 * h + 15, m4, 1)
    parts = (sums0[0], sums1[0], sums1[1], sums2[0], sums2[1], m4)
    lane = lanes()
    sub = lax.broadcasted_iota(jnp.int32, (8, NZL), 0)
    stack = jnp.zeros((8, NZL), F32)
    for i, part in enumerate(parts):
        stack = jnp.where(sub == i, jnp.sum(part, axis=0, keepdims=True), stack)
    whole = jnp.sum(stack, axis=1, keepdims=True)
    out = jnp.sum(jnp.where(lane == sub, whole, 0.0), axis=0, keepdims=True)
    row[...] = jnp.broadcast_to(out, (128, NZL))

    def traction(tile, at):
        for j, ref in enumerate((k0, k1, kp)):
            for x in range(NXL):
                r = [ref[x + 2, tile + i, at : at + 1, :] for i in range(4)]
                t[j, x : x + 1, :] = (r[0] - r[3] + 27.0 * (r[2] - r[1])) * (1.0 / 24.0)

    @pl.when(gy == 1)
    def _():
        traction(8, 7)
        sent[...] = t[:, 0:16, :]
        own[...] = t[:, 16:32, :]

    @pl.when(gy == 2)
    def _():
        traction(0, 0)
        sent[...] = t[:, 48:64, :]
        own[...] = t[:, 32:48, :]

    @pl.when(jnp.logical_or(gy == 0, gy == 3))
    def _():
        sent[...] = jnp.zeros_like(sent)
        own[...] = jnp.zeros_like(own)


def coefficients(rows):
    tot = jnp.sum(rows, axis=0, keepdims=True)
    lane = lax.broadcasted_iota(jnp.int32, (1, NZL), 1)
    v = [jnp.sum(jnp.where(lane == i, tot, 0.0), axis=1, keepdims=True) for i in range(6)]
    v0, m0, m1, m2, m3, m4 = v
    v1, v2 = m0, m1
    l1 = m1 / m0
    l2 = m2 / m0
    d1 = m2 - l1 * m1
    e = m3 - l2 * m1
    f1 = v1 - l1 * v0
    l3 = e / d1
    d2 = (m4 - l2 * m2) - l3 * e
    f2 = (v2 - l2 * v0) - l3 * f1
    c2 = f2 / d2
    c1 = (f1 - e * c2) / d1
    c0 = (v0 - m1 * c1 - m2 * c2) / m0
    return c0, c1, c2


def scaled_sinh(a, s):
    half = 0.6931471805599453
    large = jnp.exp(a - s - half) - jnp.exp(-a - s - half)
    q = a * a
    small = a * (1.0 + q * (1.0 / 6.0 + q * (1.0 / 120.0 + q * (1.0 / 5040.0)))) * jnp.exp(-s)
    return jnp.where(jnp.abs(a) < 0.5, small, large)


def final_kernel(k0, k1, k2, rows, own, got, prestress, state, normal, out, slip, buf, sem):
    gy = lax.axis_index("gy")
    parts = 4
    step = NXL // parts
    c0, c1, c2 = coefficients(rows[...])

    def copy(i):
        at = pl.ds(i * step, step)
        return pltpu.make_async_copy(buf.at[at], out.at[at], sem.at[i])

    def plane(x, carry):
        for v in range(TILES):
            at = pl.ds(v, 8, stride=TILES)
            buf[x, at, :] = c0 * k0[x + 2, v + 2] + c1 * k1[x + 2, v + 2] + c2 * k2[x + 2, v + 2]
        return carry

    for i in range(parts):
        lax.fori_loop(i * step, (i + 1) * step, plane, 0)
        copy(i).start()
    mine = jnp.logical_or(gy == 1, gy == 2)
    t = jnp.where(mine, own[...], got[...])
    traction = c0 * t[0] + c1 * t[1] + c2 * t[2]
    arg = (prestress[...] + 2.0 * traction) / normal[...]
    slip[...] = scaled_sinh(arg, state[...])
    for i in range(parts):
        copy(i).wait()


def swap(x, axes, pairs):
    return lax.ppermute(x, axes, [*pairs, *((b, a) for a, b in pairs)])


def exchange(ex, ox, ey, oy, z):
    evens = [(2 * i, 2 * i + 1) for i in range(8)]
    odds = [(2 * i + 1, (2 * i + 2) % 16) for i in range(8)]
    return (
        swap(ex, GX, evens),
        swap(ox, GX, odds),
        swap(ey, "gy", [(0, 1), (2, 3)]),
        swap(oy, "gy", [(1, 2), (3, 0)]),
        swap(z, "gz", [(0, 1)]),
    )


VM = pl.BlockSpec(memory_space=pltpu.VMEM)
HB = pl.BlockSpec(memory_space=pltpu.HBM)
BLOCK = (NXL, NYL, NZL)
TILED = (NXL, TILES, 8, NZL)
PADDED = (PX, TILES + 4, 8, NZL)
FACE = (2, TILES, 8, NZL)
FACES = (FACE, FACE, (2, NXL, NZL), (2, NXL, NZL), FACE)


def call(kernel, name, args, outs, scratch, aliases=None):
    return pl.pallas_call(
        kernel,
        out_shape=tuple(vmem(s) for s in outs),
        in_specs=[VM] * len(args),
        out_specs=(VM,) * len(outs),
        input_output_aliases=aliases or {},
        scratch_shapes=[vmem(s) for s in scratch],
        compiler_params=pltpu.CompilerParams(vmem_limit_bytes=LIMIT),
        cost_estimate=cost(),
        name=name,
    )(*map(in_vmem, args))


def cost():
    return pl.CostEstimate(flops=20_000_000, bytes_accessed=10_000_000, transcendentals=0)


def stage(name, kp, faces, zo, prev, dinv):
    return call(
        stage_kernel,
        name,
        (kp, *faces, zo, prev, dinv),
        (PADDED, PADDED, TILED, *FACES, (2, 8, NZL)),
        (FACE, (NXL + 2, TILES, 8, NZL)),
        {0: 0},
    )


def per_device(load, stiffness, prestress, state_var, normal_a):
    outs = (TILED, TILED, PADDED, *FACES, (1, 8, NZL))
    b, dinv, k0, *faces, sums0 = pl.pallas_call(
        first_kernel,
        out_shape=tuple(vmem(s) for s in outs),
        in_specs=[HB, HB],
        out_specs=(VM,) * len(outs),
        scratch_shapes=[vmem(BLOCK), vmem(BLOCK), pltpu.SemaphoreType.DMA((PARTS,)), pltpu.SemaphoreType.DMA((PARTS,))],
        compiler_params=pltpu.CompilerParams(vmem_limit_bytes=LIMIT),
        cost_estimate=cost(),
        name="start",
    )(*(pltpu.with_memory_space_constraint(x, pltpu.HBM) for x in (load, stiffness)))
    k0, k1, acc0, *faces, sums1 = stage("stage_one", k0, exchange(*faces), faces[-1], b, dinv)
    k1, k2, acc1, *faces, sums2 = stage("stage_two", k1, exchange(*faces), faces[-1], acc0, dinv)
    k2, row, own, sent = call(
        last_kernel,
        "last",
        (k2, k0, k1, *exchange(*faces), faces[-1], acc1, sums0, sums1, sums2),
        (PADDED, (128, NZL), (3, 16, NZL), (3, 16, NZL)),
        ((3, NXL, NZL), FACE, (NXL + 2, TILES, 8, NZL)),
        {0: 0},
    )
    got = swap(sent, "gy", [(0, 1), (2, 3)])
    rows = lax.all_to_all(row, ALL, 0, 0, tiled=True)
    out, slip = pl.pallas_call(
        final_kernel,
        out_shape=(jax.ShapeDtypeStruct(BLOCK, F32), jax.ShapeDtypeStruct((16, NZL), F32)),
        in_specs=[VM] * 9,
        out_specs=(HB, VM),
        scratch_shapes=[vmem(BLOCK), pltpu.SemaphoreType.DMA((4,))],
        compiler_params=pltpu.CompilerParams(vmem_limit_bytes=LIMIT),
        cost_estimate=cost(),
        name="final",
    )(*map(in_vmem, (k0, k1, k2, rows, own, got)), prestress, state_var, normal_a)
    return out, slip


def solution(mesh):
    torus = Mesh(
        mesh.devices.reshape(4, 4, mesh.shape["gy"], mesh.shape["gz"]), ("gx_0", "gx_1", "gy", "gz")
    )
    block = P(GX, "gy", "gz")
    fault = P(GX_GY, "gz")
    return jax.shard_map(
        per_device,
        mesh=torus,
        in_specs=(block, block, fault, fault, fault),
        out_specs=(block, fault),
        check_vma=False,
    )
```

```python
import functools

import jax
import jax.numpy as jnp
from jax import lax
from jax.experimental import pallas as pl
from jax.experimental.pallas import tpu as pltpu
from jax.sharding import Mesh
from jax.sharding import PartitionSpec as P

GX = ("gx_0", "gx_1")
GX_GY = ("gx_0", "gx_1", "gy")
ALL = ("gx_0", "gx_1", "gy", "gz")
F32 = jnp.float32

NXL, NYL, NZL = 64, 64, 128
PX = NXL + 4
PARTS = 8
TILES = 8
LIMIT = 6 * 2**20


def vmem(shape):
    return pltpu.VMEM(shape, F32)


def in_vmem(x):
    return pltpu.with_memory_space_constraint(x, pltpu.VMEM)


def place():
    gx = lax.axis_index("gx_0") * lax.axis_size("gx_1") + lax.axis_index("gx_1")
    return gx, lax.axis_index("gy"), lax.axis_index("gz")


def lanes():
    return lax.broadcasted_iota(jnp.int32, (8, NZL), 1)


def pack_z(x, tile, packed):
    shift = lax.rem(4 * x + 2 + NZL, NZL)
    return jnp.where(lanes() // 4 == lax.rem(x, 32), pltpu.roll(tile, shift, 1), packed)


def finish_plane(kn, x, packed):
    sub = lax.broadcasted_iota(jnp.int32, (8, NZL), 0)
    tiles = [kn[x + 2, v + 2] for v in range(TILES)]
    for i in range(2):
        kn[x + 2, i] = jnp.where(sub == 0, 0.0, pltpu.roll(tiles[6 + i], 1, 0))
        kn[x + 2, 10 + i] = jnp.where(sub == 7, 0.0, pltpu.roll(tiles[i], 7, 0))
    return tuple(pack_z(x, t, p) for t, p in zip(tiles, packed))


def zeros(n):
    return tuple(jnp.zeros((8, NZL), F32) for _ in range(n))


def total_of(parts):
    while len(parts) > 1:
        parts = [a + b for a, b in zip(parts[::2], parts[1::2])] + parts[len(parts) & ~1 :]
    return parts[0]


def clear_sides(kp):
    for x in (0, NXL + 2):
        kp[x : x + 2, 2:10] = jnp.zeros(FACE, F32)


def send_faces(kp, ex, ox, ey, oy):
    gx, gy, _ = place()
    even = lax.rem(gx, 2) == 0

    def planes(up, down):
        up[...] = kp[NXL : NXL + 2, 2:10]
        down[...] = kp[2:4, 2:10]

    @pl.when(even)
    def _():
        planes(ex, ox)

    @pl.when(jnp.logical_not(even))
    def _():
        planes(ox, ex)

    def rows(up, down):
        for x in range(NXL):
            for k in range(2):
                up[k, x : x + 1, :] = kp[x + 2, 8 + k, 7:8, :]
                down[k, x : x + 1, :] = kp[x + 2, 2 + k, 0:1, :]

    even_y = lax.rem(gy, 2) == 0

    @pl.when(even_y)
    def _():
        rows(ey, oy)

    @pl.when(jnp.logical_not(even_y))
    def _():
        rows(oy, ey)


def sides(e, o, at, last):
    even = lax.rem(at, 2) == 0
    return jnp.where(even, o, e), jnp.where(even, e, o)


def taken(e, o, at, last):
    inner = jnp.logical_and(at != 0, at != last)
    return sides(e, jnp.where(inner, o, 0.0), at, last)


def over(low, high):
    return 16.0 * low[1] - low[0], -low[1], -high[0], 16.0 * high[0] - high[1]


def z_terms(terms, z, zr):
    gz = lax.axis_index("gz")
    at = lax.rem(lanes(), 4)
    ours = (at >= 2) == (gz == 0)
    for h in range(2):
        for v in range(TILES):
            d = jnp.where(ours, zr[h, v], 0.0) - z[h, v]
            two = jnp.where(at < 2, pltpu.roll(d, NZL - 2, 1), pltpu.roll(d, 2, 1))
            one = jnp.where(at == 1, pltpu.roll(d, NZL - 1, 1), jnp.where(at == 2, pltpu.roll(d, 1, 1), 0.0))
            terms[h, v] = 16.0 * one - two


def z_part(kp, x, half, terms, out):
    lane = lanes()
    shift = lax.rem(126 + 2 * NZL - 4 * x, NZL)
    edge = jnp.logical_or(lane < 2, lane >= NZL - 2)
    for v in range(TILES):
        here = kp[x + 2, v + 2]
        near = pltpu.roll(here, 1, 1) + pltpu.roll(here, NZL - 1, 1)
        far = pltpu.roll(here, 2, 1) + pltpu.roll(here, NZL - 2, 1)
        out[x, v] = (16.0 * near - far) + jnp.where(edge, pltpu.roll(terms[half, v], shift, 1), 0.0)


def stencil(kp, x, zpart):
    p = [kp[x + 2, j] for j in range(TILES + 4)]
    for v in range(TILES):
        near = (kp[x + 1, v + 2] + kp[x + 3, v + 2]) + (p[v + 1] + p[v + 3])
        far = (kp[x, v + 2] + kp[x + 4, v + 2]) + (p[v] + p[v + 4])
        yield v, p[v + 2], (16.0 * near - far) + zpart[x, v]


def inside(kp, zo, zr, terms, zpart, plane, carry):
    z_terms(terms, zo, zr)
    for x in range(2):
        z_part(kp, x, 0, terms, zpart)

    def planes(i, carry, half, ahead=True):
        for x in (2 * i, 2 * i + 1):
            carry = plane(x, stencil(kp, x, zpart), carry)
        if ahead:
            for x in (2 * i + 2, 2 * i + 3):
                z_part(kp, x, half, terms, zpart)
        return carry

    for h in range(2):
        carry = lax.fori_loop(16 * h, 16 * h + 15, functools.partial(planes, half=h), carry)
        carry = planes(16 * h + 15, carry, 1, h == 0)
    return carry


def first_kernel(load, stiff, b, dinv, kp, ex, ox, ey, oy, z, sums, raw, s, sem_b, sem_s):
    step = NXL // PARTS

    def copies(i):
        at = pl.ds(i * step, step)
        return (
            pltpu.make_async_copy(load.at[at], raw.at[at], sem_b.at[i]),
            pltpu.make_async_copy(stiff.at[at], s.at[at], sem_s.at[i]),
        )

    for i in range(PARTS):
        for c in copies(i):
            c.start()
    clear_sides(kp)

    def planes(i, carry):
        packed, total = carry
        for x in (2 * i - 2, 2 * i - 1):
            packed = finish_plane(kp, x, packed)
        parts = []
        for x in (2 * i, 2 * i + 1):
            for v in range(TILES):
                row = pl.ds(v, 8, stride=TILES)
                inverse = 1.0 / (90.0 + 12.0 * s[x, row, :])
                right = 12.0 * raw[x, row, :]
                k = right * inverse
                b[x, v] = right
                dinv[x, v] = inverse
                kp[x + 2, v + 2] = k
                parts.append(k * right)
        return packed, total + total_of(parts)

    (total,) = zeros(1)
    packed = zeros(TILES)
    for i in range(PARTS):
        for c in copies(i):
            c.wait()
        packed, total = lax.fori_loop(i * step // 2, (i + 1) * step // 2, planes, (packed, total))
        if (i + 1) * step % 32 == 0:
            for x in ((i + 1) * step - 2, (i + 1) * step - 1):
                packed = finish_plane(kp, x, packed)
            for v in range(TILES):
                z[(i + 1) * step // 32 - 1, v] = packed[v]
    sums[0] = total
    send_faces(kp, ex, ox, ey, oy)


def inside_kernel(kp, zo, zr, out, terms):
    def plane(x, values, carry):
        for v, _, a in values:
            out[x, v] = a
        return carry

    inside(kp, zo, zr, terms, out, plane, 0)


def inside_sum_kernel(kp, zo, zr, prev, out, terms, zpart):
    def plane(x, values, total):
        return total + total_of([here * (prev[x, v] - a) for v, here, a in values])

    out[...] = inside(kp, zo, zr, terms, zpart, plane, zeros(1)[0])


def across_kernel(
    first, part, kp, prev, dinv, exr, oxr, eyr, oyr, acc, kn, ex, ox, ey, oy, z, sums, rows, tiles
):
    del part
    gx, gy, _ = place()
    sub = lax.broadcasted_iota(jnp.int32, (8, NZL), 0)
    clear_sides(kn)
    for x, extra in zip((0, 1, NXL - 2, NXL - 1), over(*taken(exr[...], oxr[...], gx, 15))):
        acc[x] = acc[x] + extra
    for j, extra in enumerate(over(*taken(eyr[...], oyr[...], gy, 3))):
        rows[j] = extra
    for x in range(NXL):
        for j in range(4):
            tiles[x, j] = jnp.where(sub == (0 if j < 2 else 7), rows[j, x : x + 1, :], 0.0)

    def planes(i, carry):
        packed, s0, s1 = carry
        for x in (2 * i - 2, 2 * i - 1):
            packed = finish_plane(kn, x, packed)
        p0, p1 = [], []
        for x in (2 * i, 2 * i + 1):
            for v in range(TILES):
                a = acc[x, v]
                if v in (0, 1, 6, 7):
                    a = a + tiles[x, v if v < 2 else v - 4]
                change = prev[x, v] - a
                new = change if first else a
                k = new * dinv[x, v]
                acc[x, v] = new
                kn[x + 2, v + 2] = k
                p0.append(kp[x + 2, v + 2] * change)
                p1.append(k * change)
        return packed, s0 + total_of(p0), s1 + total_of(p1)

    carry = (zeros(TILES), *zeros(2))
    for h in range(2):
        packed, s0, s1 = lax.fori_loop(16 * h, 16 * h + 16, planes, carry)
        for x in (32 * h + 30, 32 * h + 31):
            packed = finish_plane(kn, x, packed)
        for v in range(TILES):
            z[h, v] = packed[v]
        carry = (packed, s0, s1)
    sums[0] = s0
    sums[1] = s1
    send_faces(kn, ex, ox, ey, oy)


def last_kernel(*refs):
    sums0, sums1, sums2, part = refs[:4]
    ex, ox, ey, oy, exr, oxr, eyr, oyr = refs[4:12]
    pairs = (refs[12:14], refs[14:16], (oy, oyr))
    row, own, sent = refs[16:]
    gx, gy, _ = place()
    m4 = part[...]
    for e, o, er, orr, at, last in ((ex, ox, exr, oxr, gx, 15), (ey, oy, eyr, oyr, gy, 3)):
        low, high = sides(e[...], o[...], at, last)
        extra = over(*taken(er[...], orr[...], at, last))
        gain = low[0] * extra[0] + low[1] * extra[1] + high[0] * extra[2] + high[1] * extra[3]
        m4 = m4 - gain.reshape(8, 8, NZL).sum(axis=0)
    parts = (sums0[0], sums1[0], sums1[1], sums2[0], sums2[1], m4)
    lane = lanes()
    sub = lax.broadcasted_iota(jnp.int32, (8, NZL), 0)
    stack = jnp.zeros((8, NZL), F32)
    for i, p in enumerate(parts):
        stack = jnp.where(sub == i, jnp.sum(p, axis=0, keepdims=True), stack)
    whole = jnp.sum(stack, axis=1, keepdims=True)
    out = jnp.sum(jnp.where(lane == sub, whole, 0.0), axis=0, keepdims=True)
    row[...] = jnp.broadcast_to(out, (128, NZL))
    below = gy == 1
    for j, (mine, other) in enumerate(pairs):
        mine, other = mine[...], other[...]
        a = jnp.where(below, mine, other)
        b = jnp.where(below, other, mine)
        t = (a[0] - b[1] + 27.0 * (b[0] - a[1])) * (1.0 / 24.0)
        sent[j] = jnp.where(below, t[0:16], t[48:64])
        own[j] = jnp.where(below, t[16:32], t[32:48])


def coefficients(rows):
    tot = jnp.sum(rows, axis=0, keepdims=True)
    lane = lax.broadcasted_iota(jnp.int32, (1, NZL), 1)
    v = [jnp.sum(jnp.where(lane == i, tot, 0.0), axis=1, keepdims=True) for i in range(6)]
    v0, g00, g01, g11, g12, g22 = v
    g02 = g01 - g11
    l1 = g01 / g00
    l2 = g02 / g00
    d1 = g11 - l1 * g01
    e = g12 - l2 * g01
    f1 = g00 - l1 * v0
    l3 = e / d1
    d2 = (g22 - l2 * g02) - l3 * e
    f2 = ((g00 - g01) - l2 * v0) - l3 * f1
    c2 = f2 / d2
    c1 = (f1 - e * c2) / d1
    c0 = (v0 - g01 * c1 - g02 * c2) / g00
    return c0, c1, c2


def scaled_sinh(a, s):
    half = 0.6931471805599453
    large = jnp.exp(a - s - half) - jnp.exp(-a - s - half)
    q = a * a
    small = a * (1.0 + q * (1.0 / 6.0 + q * (1.0 / 120.0 + q * (1.0 / 5040.0)))) * jnp.exp(-s)
    return jnp.where(jnp.abs(a) < 0.5, small, large)


def final_kernel(k0, k1, k2, rows, own, got, prestress, state, normal, out, slip, buf, sem):
    gy = lax.axis_index("gy")
    parts = 4
    step = NXL // parts
    c0, c1, c2 = coefficients(rows[...])

    def copy(i):
        at = pl.ds(i * step, step)
        return pltpu.make_async_copy(buf.at[at], out.at[at], sem.at[i])

    def plane(x, carry):
        for v in range(TILES):
            at = pl.ds(v, 8, stride=TILES)
            buf[x, at, :] = c0 * k0[x + 2, v + 2] + c1 * k1[x + 2, v + 2] + c2 * k2[x + 2, v + 2]
        return carry

    for i in range(parts):
        lax.fori_loop(i * step, (i + 1) * step, plane, 0)
        copy(i).start()
    mine = jnp.logical_or(gy == 1, gy == 2)
    t = jnp.where(mine, own[...], got[...])
    traction = c0 * t[0] + c1 * t[1] + c2 * t[2]
    arg = (prestress[...] + 2.0 * traction) / normal[...]
    slip[...] = scaled_sinh(arg, state[...])
    for i in range(parts):
        copy(i).wait()


def swap(x, axes, pairs):
    return lax.ppermute(x, axes, [*pairs, *((b, a) for a, b in pairs)])


def exchange(ex, ox, ey, oy, z):
    evens = [(2 * i, 2 * i + 1) for i in range(8)]
    odds = [(2 * i + 1, (2 * i + 2) % 16) for i in range(8)]
    zr = swap(z, "gz", [(0, 1)])
    return (
        swap(ex, GX, evens),
        swap(ox, GX, odds),
        swap(ey, "gy", [(0, 1), (2, 3)]),
        swap(oy, "gy", [(1, 2), (3, 0)]),
        zr,
    )


VM = pl.BlockSpec(memory_space=pltpu.VMEM)
HB = pl.BlockSpec(memory_space=pltpu.HBM)
BLOCK = (NXL, NYL, NZL)
TILED = (NXL, TILES, 8, NZL)
PADDED = (PX, TILES + 4, 8, NZL)
FACE = (2, TILES, 8, NZL)
FACES = (FACE, FACE, (2, NXL, NZL), (2, NXL, NZL), FACE)


def call(kernel, name, args, outs, scratch, aliases=None):
    return pl.pallas_call(
        kernel,
        out_shape=tuple(vmem(s) for s in outs),
        in_specs=[VM] * len(args),
        out_specs=(VM,) * len(outs),
        input_output_aliases=aliases or {},
        scratch_shapes=[vmem(s) for s in scratch],
        compiler_params=pltpu.CompilerParams(vmem_limit_bytes=LIMIT),
        cost_estimate=cost(),
        name=name,
    )(*map(in_vmem, args))


def cost():
    return pl.CostEstimate(flops=20_000_000, bytes_accessed=10_000_000, transcendentals=0)


def across(name, k, faces, prev, dinv):
    exr, oxr, eyr, oyr, zr = exchange(*faces)
    (part,) = call(inside_kernel, name + "_inside", (k, faces[-1], zr), (TILED,), (FACE,))
    acc, kn, *rest = call(
        functools.partial(across_kernel, name == "one"),
        name + "_across",
        (part, k, prev, dinv, exr, oxr, eyr, oyr),
        (TILED, PADDED, *FACES, (2, 8, NZL)),
        ((4, NXL, NZL), (NXL, 4, 8, NZL)),
        {0: 0},
    )
    return acc, kn, rest[:-1], rest[-1], oyr


def per_device(load, stiffness, prestress, state_var, normal_a):
    outs = (TILED, TILED, PADDED, *FACES, (1, 8, NZL))
    b, dinv, k0, *faces, sums0 = pl.pallas_call(
        first_kernel,
        out_shape=tuple(vmem(s) for s in outs),
        in_specs=[HB, HB],
        out_specs=(VM,) * len(outs),
        scratch_shapes=[vmem(BLOCK), vmem(BLOCK), pltpu.SemaphoreType.DMA((PARTS,)), pltpu.SemaphoreType.DMA((PARTS,))],
        compiler_params=pltpu.CompilerParams(vmem_limit_bytes=LIMIT),
        cost_estimate=cost(),
        name="start",
    )(*(pltpu.with_memory_space_constraint(x, pltpu.HBM) for x in (load, stiffness)))
    e1, k1, faces1, sums1, oyr0 = across("one", k0, faces, b, dinv)
    e2, k2, faces2, sums2, oyr1 = across("two", k1, faces1, e1, dinv)
    exr, oxr, eyr, oyr, zr = exchange(*faces2)
    (part,) = call(
        inside_sum_kernel,
        "three_inside",
        (k2, faces2[-1], zr, e2),
        ((8, NZL),),
        (FACE, TILED),
    )
    row, own, sent = call(
        last_kernel,
        "last",
        (sums0, sums1, sums2, part, *faces2[:4], exr, oxr, eyr, oyr, faces[3], oyr0, faces1[3], oyr1),
        ((128, NZL), (3, 16, NZL), (3, 16, NZL)),
        (),
    )
    got = swap(sent, "gy", [(0, 1), (2, 3)])
    rows = lax.all_to_all(row, ALL, 0, 0, tiled=True)
    out, slip = pl.pallas_call(
        final_kernel,
        out_shape=(jax.ShapeDtypeStruct(BLOCK, F32), jax.ShapeDtypeStruct((16, NZL), F32)),
        in_specs=[VM] * 9,
        out_specs=(HB, VM),
        scratch_shapes=[vmem(BLOCK), pltpu.SemaphoreType.DMA((4,))],
        compiler_params=pltpu.CompilerParams(vmem_limit_bytes=LIMIT),
        cost_estimate=cost(),
        name="final",
    )(*map(in_vmem, (k0, k1, k2, rows, own, got)), prestress, state_var, normal_a)
    return out, slip


def solution(mesh):
    torus = Mesh(
        mesh.devices.reshape(4, 4, mesh.shape["gy"], mesh.shape["gz"]), ("gx_0", "gx_1", "gy", "gz")
    )
    block = P(GX, "gy", "gz")
    fault = P(GX_GY, "gz")
    return jax.shard_map(
        per_device,
        mesh=torus,
        in_specs=(block, block, fault, fault, fault),
        out_specs=(block, fault),
        check_vma=False,
    )
```

```python
import functools

import jax
import jax.numpy as jnp
from jax import lax
from jax.experimental import pallas as pl
from jax.experimental.pallas import tpu as pltpu
from jax.sharding import Mesh
from jax.sharding import PartitionSpec as P

GX = ("gx_0", "gx_1")
GX_GY = ("gx_0", "gx_1", "gy")
ALL = ("gx_0", "gx_1", "gy", "gz")
F32 = jnp.float32

NXL, NYL, NZL = 64, 64, 128
PX = NXL + 4
PARTS = 8
TILES = 8
LIMIT = 9 * 2**20
AT_ONCE = 4


def vmem(shape):
    return pltpu.VMEM(shape, F32)


def in_vmem(x):
    return pltpu.with_memory_space_constraint(x, pltpu.VMEM)


def in_hbm(x):
    return pltpu.with_memory_space_constraint(x, pltpu.HBM)


def place():
    gx = lax.axis_index("gx_0") * lax.axis_size("gx_1") + lax.axis_index("gx_1")
    return gx, lax.axis_index("gy"), lax.axis_index("gz")


def lanes():
    return lax.broadcasted_iota(jnp.int32, (8, NZL), 1)


def pack_z(x, tile, packed):
    shift = lax.rem(4 * x + 2 + NZL, NZL)
    return jnp.where(lanes() // 4 == lax.rem(x, 32), pltpu.roll(tile, shift, 1), packed)


def finish_plane(kn, x, packed):
    x = jnp.where(x < 0, x + AT_ONCE, x)
    sub = lax.broadcasted_iota(jnp.int32, (8, NZL), 0)
    tiles = [kn[x + 2, v + 2] for v in range(TILES)]
    for i in range(2):
        kn[x + 2, i] = jnp.where(sub == 0, 0.0, pltpu.roll(tiles[6 + i], 1, 0))
        kn[x + 2, 10 + i] = jnp.where(sub == 7, 0.0, pltpu.roll(tiles[i], 7, 0))
    return tuple(pack_z(x, t, p) for t, p in zip(tiles, packed))


def zeros(n):
    return tuple(jnp.zeros((8, NZL), F32) for _ in range(n))


def total_of(parts):
    while len(parts) > 1:
        parts = [a + b for a, b in zip(parts[::2], parts[1::2])] + parts[len(parts) & ~1 :]
    return parts[0]


def clear_sides(kp):
    for x in (0, NXL + 2):
        kp[x : x + 2, 2:10] = jnp.zeros(FACE, F32)


def send_faces(kp, ex, ox, ey, oy):
    gx, gy, _ = place()
    even = lax.rem(gx, 2) == 0

    def planes(up, down):
        up[...] = kp[NXL : NXL + 2, 2:10]
        down[...] = kp[2:4, 2:10]

    @pl.when(even)
    def _():
        planes(ex, ox)

    @pl.when(jnp.logical_not(even))
    def _():
        planes(ox, ex)

    def rows(up, down):
        for x in range(NXL):
            for k in range(2):
                up[k, x : x + 1, :] = kp[x + 2, 8 + k, 7:8, :]
                down[k, x : x + 1, :] = kp[x + 2, 2 + k, 0:1, :]

    even_y = lax.rem(gy, 2) == 0

    @pl.when(even_y)
    def _():
        rows(ey, oy)

    @pl.when(jnp.logical_not(even_y))
    def _():
        rows(oy, ey)


def sides(e, o, at, last):
    even = lax.rem(at, 2) == 0
    return jnp.where(even, o, e), jnp.where(even, e, o)


def taken(e, o, at, last):
    inner = jnp.logical_and(at != 0, at != last)
    return sides(e, jnp.where(inner, o, 0.0), at, last)


def over(low, high):
    return 16.0 * low[1] - low[0], -low[1], -high[0], 16.0 * high[0] - high[1]


def z_terms(terms, z, zr):
    gz = lax.axis_index("gz")
    at = lax.rem(lanes(), 4)
    ours = (at >= 2) == (gz == 0)
    for h in range(2):
        for v in range(TILES):
            d = jnp.where(ours, zr[h, v], 0.0) - z[h, v]
            two = jnp.where(at < 2, pltpu.roll(d, NZL - 2, 1), pltpu.roll(d, 2, 1))
            one = jnp.where(at == 1, pltpu.roll(d, NZL - 1, 1), jnp.where(at == 2, pltpu.roll(d, 1, 1), 0.0))
            terms[h, v] = 16.0 * one - two


def stencil(kp, x, zpart):
    p = [kp[x + 2, j] for j in range(TILES + 4)]
    for v in range(TILES):
        near = (kp[x + 1, v + 2] + kp[x + 3, v + 2]) + (p[v + 1] + p[v + 3])
        far = (kp[x, v + 2] + kp[x + 4, v + 2]) + (p[v] + p[v + 4])
        yield v, (16.0 * near - far) + zpart[x, v]


def inside_kernel(kp, zo, zr, out, terms, one, three, zpart):
    z_terms(terms, zo, zr)
    lane = lanes()
    edge = jnp.logical_or(lane < 2, lane >= NZL - 2)

    def shift_one(x):
        x = jnp.minimum(x, NXL - 1)
        for v in range(TILES):
            one[x, v] = pltpu.roll(kp[x + 2, v + 2], 1, 1)

    def shift_three(x):
        x = jnp.minimum(x, NXL - 1)
        for v in range(TILES):
            three[x, v] = pltpu.roll(16.0 * kp[x + 2, v + 2] - one[x, v], 3, 1)

    def shift_back(x):
        x = jnp.minimum(x, NXL - 1)
        half = x // 32
        back = lax.rem(126 + 2 * NZL - 4 * x, NZL)
        for v in range(TILES):
            w = (16.0 * one[x, v] - kp[x + 2, v + 2]) + three[x, v]
            side = jnp.where(edge, pltpu.roll(terms[half, v], back, 1), 0.0)
            zpart[x, v] = pltpu.roll(w, NZL - 2, 1) + side

    def ahead(i, stages):
        for stage, first in stages:
            for x in (first, first + 1):
                stage(2 * i + x)

    for i in range(3):
        ahead(i, ((shift_one, 0),))
    for i in range(2):
        ahead(i, ((shift_three, 0),))
    ahead(0, ((shift_back, 0),))

    def planes(i, carry):
        for x in (2 * i, 2 * i + 1):
            for v, a in stencil(kp, x, zpart):
                out[x, v] = a
        ahead(i, ((shift_back, 2), (shift_three, 4), (shift_one, 6)))
        return carry

    lax.fori_loop(0, NXL // 2, planes, 0)


def inside_sum_kernel(kp, prev, out, zpart):
    def shift(x):
        x = jnp.minimum(x, NXL - 1)
        for v in range(TILES):
            here = kp[x + 2, v + 2]
            zpart[x, v] = 16.0 * pltpu.roll(here, NZL - 1, 1) - pltpu.roll(here, NZL - 2, 1)

    for x in range(2):
        shift(x)

    def planes(i, total):
        parts = []
        for x in (2 * i, 2 * i + 1):
            p = [kp[x + 2, j] for j in range(2, TILES + 4)]
            for v in range(TILES):
                near = kp[x + 3, v + 2] + p[v + 1]
                far = kp[x + 4, v + 2] + p[v + 2]
                a = (16.0 * near - far) + zpart[x, v]
                parts.append(p[v] * (prev[x, v] - 2.0 * a))
        for x in (2 * i + 2, 2 * i + 3):
            shift(x)
        return total + total_of(parts)

    out[...] = lax.fori_loop(0, NXL // 2, planes, zeros(1)[0])


def z_pairs(z, zr):
    gz = lax.axis_index("gz")
    at = lax.rem(lanes(), 4)
    parts = []
    for h in range(2):
        for v in range(TILES):
            own, other = z[h, v], zr[h, v]
            up = 2.0 * own - jnp.where(gz == 0, other, 0.0)
            down = jnp.where(gz == 0, 0.0, -other)
            up = jnp.where(at == 1, 16.0 * pltpu.roll(up, NZL - 1, 1), 0.0) - pltpu.roll(up, NZL - 2, 1)
            down = jnp.where(at == 2, 16.0 * pltpu.roll(down, 1, 1), 0.0) - pltpu.roll(down, 2, 1)
            parts.append(own * jnp.where(at < 2, up, down))
    return total_of(parts)


def first_kernel(load, stiff, b, dinv, kp, ex, ox, ey, oy, z, sums, raw, s, sem_b, sem_s):
    step = NXL // PARTS

    def copies(i):
        at = pl.ds(i * step, step)
        return (
            pltpu.make_async_copy(load.at[at], raw.at[at], sem_b.at[i]),
            pltpu.make_async_copy(stiff.at[at], s.at[at], sem_s.at[i]),
        )

    for i in range(PARTS):
        for c in copies(i):
            c.start()
    clear_sides(kp)

    def planes(i, carry):
        packed, total = carry
        for x in range(AT_ONCE):
            packed = finish_plane(kp, AT_ONCE * (i - 1) + x, packed)
        parts = []
        for x in [AT_ONCE * i + x for x in range(AT_ONCE)]:
            for v in range(TILES):
                row = pl.ds(v, 8, stride=TILES)
                inverse = 1.0 / (90.0 + 12.0 * s[x, row, :])
                right = 12.0 * raw[x, row, :]
                k = right * inverse
                b[x, v] = right
                dinv[x, v] = inverse
                kp[x + 2, v + 2] = k
                parts.append(k * right)
        return packed, total + total_of(parts)

    (total,) = zeros(1)
    packed = zeros(TILES)
    for i in range(PARTS):
        for c in copies(i):
            c.wait()
        packed, total = lax.fori_loop(i * step // AT_ONCE, (i + 1) * step // AT_ONCE, planes, (packed, total))
        if (i + 1) * step % 32 == 0:
            for x in range(AT_ONCE):
                packed = finish_plane(kp, (i + 1) * step - AT_ONCE + x, packed)
            for v in range(TILES):
                z[(i + 1) * step // 32 - 1, v] = packed[v]
    sums[0] = total
    send_faces(kp, ex, ox, ey, oy)


def across_kernel(
    first, part, kp, prev, dinv, exr, oxr, eyr, oyr, acc, kn, ex, ox, ey, oy, z, sums, rows, tiles
):
    del part
    gx, gy, _ = place()
    sub = lax.broadcasted_iota(jnp.int32, (8, NZL), 0)
    clear_sides(kn)
    for x, extra in zip((0, 1, NXL - 2, NXL - 1), over(*taken(exr[...], oxr[...], gx, 15))):
        acc[x] = acc[x] + extra
    for j, extra in enumerate(over(*taken(eyr[...], oyr[...], gy, 3))):
        rows[j] = extra
    for x in range(NXL):
        for j in range(4):
            tiles[x, j] = jnp.where(sub == (0 if j < 2 else 7), rows[j, x : x + 1, :], 0.0)

    def planes(i, carry):
        packed, s0, s1 = carry
        for x in range(AT_ONCE):
            packed = finish_plane(kn, AT_ONCE * (i - 1) + x, packed)
        p0, p1 = [], []
        for x in [AT_ONCE * i + x for x in range(AT_ONCE)]:
            for v in range(TILES):
                a = acc[x, v]
                if v in (0, 1, 6, 7):
                    a = a + tiles[x, v if v < 2 else v - 4]
                change = prev[x, v] - a
                new = change if first else a
                k = new * dinv[x, v]
                acc[x, v] = new
                kn[x + 2, v + 2] = k
                p0.append(kp[x + 2, v + 2] * change)
                p1.append(k * change)
        return packed, s0 + total_of(p0), s1 + total_of(p1)

    carry = (zeros(TILES), *zeros(2))
    for h in range(2):
        steps = 32 // AT_ONCE
        packed, s0, s1 = lax.fori_loop(steps * h, steps * h + steps, planes, carry)
        for x in range(AT_ONCE):
            packed = finish_plane(kn, 32 * h + 32 - AT_ONCE + x, packed)
        for v in range(TILES):
            z[h, v] = packed[v]
        carry = (packed, s0, s1)
    sums[0] = s0
    sums[1] = s1
    send_faces(kn, ex, ox, ey, oy)


def last_kernel(*refs):
    sums0, sums1, sums2, part = refs[:4]
    ex, ox, ey, oy, z, exr, oxr, eyr, oyr, zr = refs[4:14]
    pairs = (refs[14:16], refs[16:18], (oy, oyr))
    row, own, sent = refs[18:]
    gx, gy, _ = place()
    m4 = part[...] + z_pairs(z, zr)
    for e, o, er, orr, at, last in ((ex, ox, exr, oxr, gx, 15), (ey, oy, eyr, oyr, gy, 3)):
        low, high = sides(e[...], o[...], at, last)
        extra = over(*taken(er[...], orr[...], at, last))
        gain = low[0] * extra[0] + low[1] * extra[1] + high[0] * extra[2] + high[1] * extra[3]
        m4 = m4 - gain.reshape(8, 8, NZL).sum(axis=0)
    parts = (sums0[0], sums1[0], sums1[1], sums2[0], sums2[1], m4)
    lane = lanes()
    sub = lax.broadcasted_iota(jnp.int32, (8, NZL), 0)
    stack = jnp.zeros((8, NZL), F32)
    for i, p in enumerate(parts):
        stack = jnp.where(sub == i, jnp.sum(p, axis=0, keepdims=True), stack)
    whole = jnp.sum(stack, axis=1, keepdims=True)
    out = jnp.sum(jnp.where(lane == sub, whole, 0.0), axis=0, keepdims=True)
    row[...] = jnp.broadcast_to(out, (128, NZL))
    below = gy == 1
    for j, (mine, other) in enumerate(pairs):
        mine, other = mine[...], other[...]
        a = jnp.where(below, mine, other)
        b = jnp.where(below, other, mine)
        t = (a[0] - b[1] + 27.0 * (b[0] - a[1])) * (1.0 / 24.0)
        sent[j] = jnp.where(below, t[0:16], t[48:64])
        own[j] = jnp.where(below, t[16:32], t[32:48])


def coefficients(rows):
    tot = jnp.sum(rows, axis=0, keepdims=True)
    lane = lax.broadcasted_iota(jnp.int32, (1, NZL), 1)
    v = [jnp.sum(jnp.where(lane == i, tot, 0.0), axis=1, keepdims=True) for i in range(6)]
    v0, g00, g01, g11, g12, g22 = v
    g02 = g01 - g11
    l1 = g01 / g00
    l2 = g02 / g00
    d1 = g11 - l1 * g01
    e = g12 - l2 * g01
    f1 = g00 - l1 * v0
    l3 = e / d1
    d2 = (g22 - l2 * g02) - l3 * e
    f2 = ((g00 - g01) - l2 * v0) - l3 * f1
    c2 = f2 / d2
    c1 = (f1 - e * c2) / d1
    c0 = (v0 - g01 * c1 - g02 * c2) / g00
    return c0, c1, c2


def scaled_sinh(a, s):
    half = 0.6931471805599453
    large = jnp.exp(a - s - half) - jnp.exp(-a - s - half)
    q = a * a
    small = a * (1.0 + q * (1.0 / 6.0 + q * (1.0 / 120.0 + q * (1.0 / 5040.0)))) * jnp.exp(-s)
    return jnp.where(jnp.abs(a) < 0.5, small, large)


def final_kernel(
    k0, k2, k1, rows, own, got, prestress, state, normal, out, slip, r0, r2, buf, sem0, sem2, sem
):
    gy = lax.axis_index("gy")
    step = NXL // PARTS

    def reads(i):
        at = pl.ds(2 + i * step, step)
        to = pl.ds(i * step, step)
        return (
            pltpu.make_async_copy(k0.at[at, pl.ds(2, TILES)], r0.at[to], sem0.at[i]),
            pltpu.make_async_copy(k2.at[at, pl.ds(2, TILES)], r2.at[to], sem2.at[i]),
        )

    def write(i):
        at = pl.ds(i * step, step)
        return pltpu.make_async_copy(buf.at[at], out.at[at], sem.at[i])

    for i in range(PARTS):
        for c in reads(i):
            c.start()
    c0, c1, c2 = coefficients(rows[...])

    def plane(x, carry):
        for v in range(TILES):
            at = pl.ds(v, 8, stride=TILES)
            buf[x, at, :] = c0 * r0[x, v] + c1 * k1[x + 2, v + 2] + c2 * r2[x, v]
        return carry

    for i in range(PARTS):
        for c in reads(i):
            c.wait()
        lax.fori_loop(i * step, (i + 1) * step, plane, 0)
        write(i).start()
    mine = jnp.logical_or(gy == 1, gy == 2)
    t = jnp.where(mine, own[...], got[...])
    traction = c0 * t[0] + c1 * t[1] + c2 * t[2]
    arg = (prestress[...] + 2.0 * traction) / normal[...]
    slip[...] = scaled_sinh(arg, state[...])
    for i in range(PARTS):
        write(i).wait()


def swap(x, axes, pairs):
    return lax.ppermute(x, axes, [*pairs, *((b, a) for a, b in pairs)])


def exchange(ex, ox, ey, oy, z):
    evens = [(2 * i, 2 * i + 1) for i in range(8)]
    odds = [(2 * i + 1, (2 * i + 2) % 16) for i in range(8)]
    zr = swap(z, "gz", [(0, 1)])
    return (
        swap(ex, GX, evens),
        swap(ox, GX, odds),
        swap(ey, "gy", [(0, 1), (2, 3)]),
        swap(oy, "gy", [(1, 2), (3, 0)]),
        zr,
    )


VM = pl.BlockSpec(memory_space=pltpu.VMEM)
HB = pl.BlockSpec(memory_space=pltpu.HBM)
BLOCK = (NXL, NYL, NZL)
TILED = (NXL, TILES, 8, NZL)
PADDED = (PX, TILES + 4, 8, NZL)
FACE = (2, TILES, 8, NZL)
FACES = (FACE, FACE, (2, NXL, NZL), (2, NXL, NZL), FACE)


def call(kernel, name, args, outs, scratch, aliases=None):
    return pl.pallas_call(
        kernel,
        out_shape=tuple(vmem(s) for s in outs),
        in_specs=[VM] * len(args),
        out_specs=(VM,) * len(outs),
        input_output_aliases=aliases or {},
        scratch_shapes=[vmem(s) for s in scratch],
        compiler_params=pltpu.CompilerParams(vmem_limit_bytes=LIMIT),
        cost_estimate=cost(),
        name=name,
    )(*map(in_vmem, args))


def cost():
    return pl.CostEstimate(flops=20_000_000, bytes_accessed=10_000_000, transcendentals=0)


def across(name, k, faces, prev, dinv):
    exr, oxr, eyr, oyr, zr = exchange(*faces)
    (part,) = call(inside_kernel, name + "_inside", (k, faces[-1], zr), (TILED,), (FACE, TILED, TILED, TILED))
    acc, kn, *rest = call(
        functools.partial(across_kernel, name == "one"),
        name + "_across",
        (part, k, prev, dinv, exr, oxr, eyr, oyr),
        (TILED, PADDED, *FACES, (2, 8, NZL)),
        ((4, NXL, NZL), (NXL, 4, 8, NZL)),
        {0: 0},
    )
    return acc, kn, rest[:-1], rest[-1], oyr


def per_device(load, stiffness, prestress, state_var, normal_a):
    outs = (TILED, TILED, PADDED, *FACES, (1, 8, NZL))
    b, dinv, k0, *faces, sums0 = pl.pallas_call(
        first_kernel,
        out_shape=tuple(vmem(s) for s in outs),
        in_specs=[HB, HB],
        out_specs=(VM,) * len(outs),
        scratch_shapes=[vmem(BLOCK), vmem(BLOCK), pltpu.SemaphoreType.DMA((PARTS,)), pltpu.SemaphoreType.DMA((PARTS,))],
        compiler_params=pltpu.CompilerParams(vmem_limit_bytes=LIMIT),
        cost_estimate=cost(),
        name="start",
    )(in_hbm(load), in_hbm(stiffness))
    e1, k1, faces1, sums1, oyr0 = across("one", k0, faces, b, dinv)
    e2, k2, faces2, sums2, oyr1 = across("two", k1, faces1, e1, dinv)
    taken2 = exchange(*faces2)
    (part,) = call(inside_sum_kernel, "three_inside", (k2, e2), ((8, NZL),), (TILED,))
    row, own, sent = call(
        last_kernel,
        "last",
        (sums0, sums1, sums2, part, *faces2, *taken2, faces[3], oyr0, faces1[3], oyr1),
        ((128, NZL), (3, 16, NZL), (3, 16, NZL)),
        (),
    )
    got = swap(sent, "gy", [(0, 1), (2, 3)])
    rows = lax.all_to_all(row, ALL, 0, 0, tiled=True)
    out, slip = pl.pallas_call(
        final_kernel,
        out_shape=(jax.ShapeDtypeStruct(BLOCK, F32), jax.ShapeDtypeStruct((16, NZL), F32)),
        in_specs=[HB] * 2 + [VM] * 7,
        out_specs=(HB, VM),
        scratch_shapes=[vmem(TILED), vmem(TILED), vmem(BLOCK)] + [pltpu.SemaphoreType.DMA((PARTS,))] * 3,
        compiler_params=pltpu.CompilerParams(vmem_limit_bytes=LIMIT),
        cost_estimate=cost(),
        name="final",
    )(*map(in_hbm, (k0, k2)), *map(in_vmem, (k1, rows, own, got)), prestress, state_var, normal_a)
    return out, slip


def solution(mesh):
    torus = Mesh(
        mesh.devices.reshape(4, 4, mesh.shape["gy"], mesh.shape["gz"]), ("gx_0", "gx_1", "gy", "gz")
    )
    block = P(GX, "gy", "gz")
    fault = P(GX_GY, "gz")
    return jax.shard_map(
        per_device,
        mesh=torus,
        in_specs=(block, block, fault, fault, fault),
        out_specs=(block, fault),
        check_vma=False,
    )
```

```python
import functools

import jax
import jax.numpy as jnp
from jax import lax
from jax.experimental import pallas as pl
from jax.experimental.pallas import tpu as pltpu
from jax.sharding import Mesh
from jax.sharding import PartitionSpec as P

GX = ("gx_0", "gx_1")
GX_GY = ("gx_0", "gx_1", "gy")
ALL = ("gx_0", "gx_1", "gy", "gz")
F32 = jnp.float32

NXL, NYL, NZL = 64, 64, 128
PX = NXL + 4
PARTS = 8
TILES = 8
LIMIT = 9 * 2**20
AHEAD = 8
AT_ONCE = 8


def vmem(shape):
    return pltpu.VMEM(shape, F32)


def in_vmem(x):
    return pltpu.with_memory_space_constraint(x, pltpu.VMEM)


def in_hbm(x):
    return pltpu.with_memory_space_constraint(x, pltpu.HBM)


def place():
    gx = lax.axis_index("gx_0") * lax.axis_size("gx_1") + lax.axis_index("gx_1")
    return gx, lax.axis_index("gy"), lax.axis_index("gz")


def lanes():
    return lax.broadcasted_iota(jnp.int32, (8, NZL), 1)


def pack_z(x, tile, packed):
    shift = (4 * x + 2) & (NZL - 1)
    return jnp.where(lanes() // 4 == (x & 31), pltpu.roll(tile, shift, 1), packed)


def finish_plane(kn, x, packed):
    sub = lax.broadcasted_iota(jnp.int32, (8, NZL), 0)
    tiles = [kn[x + 2, v + 2] for v in range(TILES)]
    for i in range(2):
        kn[x + 2, i] = jnp.where(sub == 0, 0.0, pltpu.roll(tiles[6 + i], 1, 0))
        kn[x + 2, 10 + i] = jnp.where(sub == 7, 0.0, pltpu.roll(tiles[i], 7, 0))
    return tuple(pack_z(x, t, p) for t, p in zip(tiles, packed))


def zeros(n):
    return tuple(jnp.zeros((8, NZL), F32) for _ in range(n))


class Total:
    def __init__(self):
        self.chains = [None] * 4
        self.count = 0

    def add(self, term):
        at = self.count % 4
        self.chains[at] = term if self.chains[at] is None else self.chains[at] + term
        self.count += 1

    def value(self):
        a, b, c, d = self.chains
        return (a + b) + (c + d)


def clear_sides(kp):
    for x in (0, NXL + 2):
        kp[x : x + 2, 2:10] = jnp.zeros(FACE, F32)


def send_faces(kp, ex, ox, ey, oy):
    gx, gy, _ = place()
    even = lax.rem(gx, 2) == 0

    def planes(up, down):
        up[...] = kp[NXL : NXL + 2, 2:10]
        down[...] = kp[2:4, 2:10]

    @pl.when(even)
    def _():
        planes(ex, ox)

    @pl.when(jnp.logical_not(even))
    def _():
        planes(ox, ex)

    def rows(up, down):
        for x in range(NXL):
            for k in range(2):
                up[k, x : x + 1, :] = kp[x + 2, 8 + k, 7:8, :]
                down[k, x : x + 1, :] = kp[x + 2, 2 + k, 0:1, :]

    even_y = lax.rem(gy, 2) == 0

    @pl.when(even_y)
    def _():
        rows(ey, oy)

    @pl.when(jnp.logical_not(even_y))
    def _():
        rows(oy, ey)


def sides(e, o, at, last):
    even = lax.rem(at, 2) == 0
    return jnp.where(even, o, e), jnp.where(even, e, o)


def taken(e, o, at, last):
    inner = jnp.logical_and(at != 0, at != last)
    return sides(e, jnp.where(inner, o, 0.0), at, last)


def over(low, high):
    return 16.0 * low[1] - low[0], -low[1], -high[0], 16.0 * high[0] - high[1]


def z_terms(terms, z, zr):
    gz = lax.axis_index("gz")
    at = lax.rem(lanes(), 4)
    ours = (at >= 2) == (gz == 0)
    for h in range(2):
        for v in range(TILES):
            d = jnp.where(ours, zr[h, v], 0.0) - z[h, v]
            two = jnp.where(at < 2, pltpu.roll(d, NZL - 2, 1), pltpu.roll(d, 2, 1))
            one = jnp.where(at == 1, pltpu.roll(d, NZL - 1, 1), jnp.where(at == 2, pltpu.roll(d, 1, 1), 0.0))
            terms[h, v] = 16.0 * one - two


def stencil(kp, x, zpart):
    p = [kp[x + 2, j] for j in range(TILES + 4)]
    for v in range(TILES):
        near = (kp[x + 1, v + 2] + kp[x + 3, v + 2]) + (p[v + 1] + p[v + 3])
        far = (kp[x, v + 2] + kp[x + 4, v + 2]) + (p[v] + p[v + 4])
        yield v, (16.0 * near - far) + zpart[x, v]


def inside_kernel(kp, zo, zr, out, terms, one, three, zpart):
    z_terms(terms, zo, zr)
    lane = lanes()
    edge = jnp.logical_or(lane < 2, lane >= NZL - 2)

    def shift_one(x, _):
        return one, x, [pltpu.roll(kp[x + 2, v + 2], 1, 1) for v in range(TILES)]

    def shift_three(x, _):
        return three, x, [pltpu.roll(16.0 * kp[x + 2, v + 2] - one[x, v], 3, 1) for v in range(TILES)]

    def shift_back(x, half):
        back = (126 - 4 * x) & (NZL - 1)
        new = []
        for v in range(TILES):
            w = (16.0 * one[x, v] - kp[x + 2, v + 2]) + three[x, v]
            side = jnp.where(edge, pltpu.roll(terms[half, v], back, 1), 0.0)
            new.append(pltpu.roll(w, NZL - 2, 1) + side)
        return zpart, x, new

    def begin(i, stages):
        begun = []
        for stage, steps in stages:
            half = lax.shift_right_logical(jnp.int32(i + steps), (32 // AHEAD).bit_length() - 1)
            begun += [stage(AHEAD * (i + steps) + x, half) for x in range(AHEAD)]
        return begun

    def end(begun):
        for ref, x, new in begun:
            for v in range(TILES):
                ref[x, v] = new[v]

    for i in range(3):
        end(begin(i, ((shift_one, 0),)))
    for i in range(2):
        end(begin(i, ((shift_three, 0),)))
    end(begin(0, ((shift_back, 0),)))

    stages = ((shift_back, 1), (shift_three, 2), (shift_one, 3))
    steps = NXL // AHEAD

    def planes(i, carry, stages=stages):
        begun = begin(i, stages)
        for x in range(AHEAD):
            x = AHEAD * i + x
            for v, a in list(stencil(kp, x, zpart)):
                out[x, v] = a
        end(begun)
        return carry

    lax.fori_loop(0, steps - 3, planes, 0)
    for i in (steps - 3, steps - 2, steps - 1):
        planes(i, 0, tuple(s for s in stages if i + s[1] < steps))


def inside_sum_kernel(kp, prev, out, zpart):
    def shift(x):
        here = [kp[x + 2, v + 2] for v in range(TILES)]
        return x, [16.0 * pltpu.roll(h, NZL - 1, 1) - pltpu.roll(h, NZL - 2, 1) for h in here]

    def end(begun):
        for x, new in begun:
            for v in range(TILES):
                zpart[x, v] = new[v]

    end([shift(x) for x in range(AHEAD)])

    steps = NXL // AHEAD

    def planes(i, total, ahead=True):
        begun = [shift(AHEAD * (i + 1) + x) for x in range(AHEAD if ahead else 0)]
        parts = Total()
        for x in [AHEAD * i + x for x in range(AHEAD)]:
            p = [kp[x + 2, j] for j in range(2, TILES + 4)]
            for v in range(TILES):
                near = kp[x + 3, v + 2] + p[v + 1]
                far = kp[x + 4, v + 2] + p[v + 2]
                a = (16.0 * near - far) + zpart[x, v]
                parts.add(p[v] * (prev[x, v] - 2.0 * a))
        end(begun)
        return total + parts.value()

    out[...] = planes(steps - 1, lax.fori_loop(0, steps - 1, planes, zeros(1)[0]), False)


def z_pairs(z, zr):
    gz = lax.axis_index("gz")
    at = lax.rem(lanes(), 4)
    parts = Total()
    for h in range(2):
        for v in range(TILES):
            own, other = z[h, v], zr[h, v]
            up = 2.0 * own - jnp.where(gz == 0, other, 0.0)
            down = jnp.where(gz == 0, 0.0, -other)
            up = jnp.where(at == 1, 16.0 * pltpu.roll(up, NZL - 1, 1), 0.0) - pltpu.roll(up, NZL - 2, 1)
            down = jnp.where(at == 2, 16.0 * pltpu.roll(down, 1, 1), 0.0) - pltpu.roll(down, 2, 1)
            parts.add(own * jnp.where(at < 2, up, down))
    return parts.value()


def first_kernel(load, stiff, b, dinv, kp, ex, ox, ey, oy, z, sums, raw, s, sem_b, sem_s):
    step = NXL // PARTS

    def copies(i):
        at = pl.ds(i * step, step)
        return (
            pltpu.make_async_copy(load.at[at], raw.at[at], sem_b.at[i]),
            pltpu.make_async_copy(stiff.at[at], s.at[at], sem_s.at[i]),
        )

    for i in range(PARTS):
        for c in copies(i):
            c.start()
    clear_sides(kp)

    def planes(i, carry):
        packed, total = carry
        for x in range(AT_ONCE):
            packed = finish_plane(kp, AT_ONCE * jnp.maximum(i - 1, 0) + x, packed)
        parts = Total()
        for x in [AT_ONCE * i + x for x in range(AT_ONCE)]:
            for v in range(TILES):
                row = pl.ds(v, 8, stride=TILES)
                inverse = 1.0 / (90.0 + 12.0 * s[x, row, :])
                right = 12.0 * raw[x, row, :]
                k = right * inverse
                b[x, v] = right
                dinv[x, v] = inverse
                kp[x + 2, v + 2] = k
                parts.add(k * right)
        return packed, total + parts.value()

    (total,) = zeros(1)
    packed = zeros(TILES)
    for i in range(PARTS):
        for c in copies(i):
            c.wait()
        packed, total = lax.fori_loop(i * step // AT_ONCE, (i + 1) * step // AT_ONCE, planes, (packed, total))
        if (i + 1) * step % 32 == 0:
            for x in range(AT_ONCE):
                packed = finish_plane(kp, (i + 1) * step - AT_ONCE + x, packed)
            for v in range(TILES):
                z[(i + 1) * step // 32 - 1, v] = packed[v]
    sums[0] = total
    send_faces(kp, ex, ox, ey, oy)


def across_kernel(
    first, part, kp, prev, dinv, exr, oxr, eyr, oyr, acc, kn, ex, ox, ey, oy, z, sums, rows, tiles
):
    del part
    gx, gy, _ = place()
    sub = lax.broadcasted_iota(jnp.int32, (8, NZL), 0)
    clear_sides(kn)
    for x, extra in zip((0, 1, NXL - 2, NXL - 1), over(*taken(exr[...], oxr[...], gx, 15))):
        acc[x] = acc[x] + extra
    for j, extra in enumerate(over(*taken(eyr[...], oyr[...], gy, 3))):
        rows[j] = extra
    for x in range(NXL):
        for j in range(4):
            tiles[x, j] = jnp.where(sub == (0 if j < 2 else 7), rows[j, x : x + 1, :], 0.0)

    def planes(i, carry):
        packed, s0, s1 = carry
        for x in range(AT_ONCE):
            packed = finish_plane(kn, AT_ONCE * jnp.maximum(i - 1, 0) + x, packed)
        p0, p1 = Total(), Total()
        for x in [AT_ONCE * i + x for x in range(AT_ONCE)]:
            for v in range(TILES):
                a = acc[x, v]
                if v in (0, 1, 6, 7):
                    a = a + tiles[x, v if v < 2 else v - 4]
                change = prev[x, v] - a
                new = change if first else a
                k = new * dinv[x, v]
                acc[x, v] = new
                kn[x + 2, v + 2] = k
                p0.add(kp[x + 2, v + 2] * change)
                p1.add(k * change)
        return packed, s0 + p0.value(), s1 + p1.value()

    carry = (zeros(TILES), *zeros(2))
    for h in range(2):
        steps = 32 // AT_ONCE
        packed, s0, s1 = lax.fori_loop(steps * h, steps * h + steps, planes, carry)
        for x in range(AT_ONCE):
            packed = finish_plane(kn, 32 * h + 32 - AT_ONCE + x, packed)
        for v in range(TILES):
            z[h, v] = packed[v]
        carry = (packed, s0, s1)
    sums[0] = s0
    sums[1] = s1
    send_faces(kn, ex, ox, ey, oy)


def last_kernel(*refs):
    sums0, sums1, sums2, part = refs[:4]
    ex, ox, ey, oy, z, exr, oxr, eyr, oyr, zr = refs[4:14]
    pairs = (refs[14:16], refs[16:18], (oy, oyr))
    row, own, sent = refs[18:]
    gx, gy, _ = place()
    m4 = part[...] + z_pairs(z, zr)
    for e, o, er, orr, at, last in ((ex, ox, exr, oxr, gx, 15), (ey, oy, eyr, oyr, gy, 3)):
        low, high = sides(e[...], o[...], at, last)
        extra = over(*taken(er[...], orr[...], at, last))
        gain = low[0] * extra[0] + low[1] * extra[1] + high[0] * extra[2] + high[1] * extra[3]
        m4 = m4 - gain.reshape(8, 8, NZL).sum(axis=0)
    parts = (sums0[0], sums1[0], sums1[1], sums2[0], sums2[1], m4)
    lane = lanes()
    sub = lax.broadcasted_iota(jnp.int32, (8, NZL), 0)
    stack = jnp.zeros((8, NZL), F32)
    for i, p in enumerate(parts):
        stack = jnp.where(sub == i, jnp.sum(p, axis=0, keepdims=True), stack)
    whole = jnp.sum(stack, axis=1, keepdims=True)
    out = jnp.sum(jnp.where(lane == sub, whole, 0.0), axis=0, keepdims=True)
    row[...] = jnp.broadcast_to(out, (128, NZL))
    below = gy == 1
    for j, (mine, other) in enumerate(pairs):
        mine, other = mine[...], other[...]
        a = jnp.where(below, mine, other)
        b = jnp.where(below, other, mine)
        t = (a[0] - b[1] + 27.0 * (b[0] - a[1])) * (1.0 / 24.0)
        sent[j] = jnp.where(below, t[0:16], t[48:64])
        own[j] = jnp.where(below, t[16:32], t[32:48])


def coefficients(rows):
    tot = jnp.sum(rows, axis=0, keepdims=True)
    lane = lax.broadcasted_iota(jnp.int32, (1, NZL), 1)
    v = [jnp.sum(jnp.where(lane == i, tot, 0.0), axis=1, keepdims=True) for i in range(6)]
    v0, g00, g01, g11, g12, g22 = v
    g02 = g01 - g11
    l1 = g01 / g00
    l2 = g02 / g00
    d1 = g11 - l1 * g01
    e = g12 - l2 * g01
    f1 = g00 - l1 * v0
    l3 = e / d1
    d2 = (g22 - l2 * g02) - l3 * e
    f2 = ((g00 - g01) - l2 * v0) - l3 * f1
    c2 = f2 / d2
    c1 = (f1 - e * c2) / d1
    c0 = (v0 - g01 * c1 - g02 * c2) / g00
    return c0, c1, c2


def scaled_sinh(a, s):
    half = 0.6931471805599453
    large = jnp.exp(a - s - half) - jnp.exp(-a - s - half)
    q = a * a
    small = a * (1.0 + q * (1.0 / 6.0 + q * (1.0 / 120.0 + q * (1.0 / 5040.0)))) * jnp.exp(-s)
    return jnp.where(jnp.abs(a) < 0.5, small, large)


def final_kernel(
    k0, k2, k1, rows, own, got, prestress, state, normal, out, slip, r0, r2, buf, sem0, sem2, sem
):
    gy = lax.axis_index("gy")
    step = NXL // PARTS

    def reads(i):
        at = pl.ds(2 + i * step, step)
        to = pl.ds(i * step, step)
        return (
            pltpu.make_async_copy(k0.at[at, pl.ds(2, TILES)], r0.at[to], sem0.at[i]),
            pltpu.make_async_copy(k2.at[at, pl.ds(2, TILES)], r2.at[to], sem2.at[i]),
        )

    def write(i):
        at = pl.ds(i * step, step)
        return pltpu.make_async_copy(buf.at[at], out.at[at], sem.at[i])

    for i in range(PARTS):
        for c in reads(i):
            c.start()
    c0, c1, c2 = coefficients(rows[...])

    def plane(x, carry):
        for v in range(TILES):
            at = pl.ds(v, 8, stride=TILES)
            buf[x, at, :] = c0 * r0[x, v] + c1 * k1[x + 2, v + 2] + c2 * r2[x, v]
        return carry

    for i in range(PARTS):
        for c in reads(i):
            c.wait()
        lax.fori_loop(i * step, (i + 1) * step, plane, 0)
        write(i).start()
    mine = jnp.logical_or(gy == 1, gy == 2)
    t = jnp.where(mine, own[...], got[...])
    traction = c0 * t[0] + c1 * t[1] + c2 * t[2]
    arg = (prestress[...] + 2.0 * traction) / normal[...]
    slip[...] = scaled_sinh(arg, state[...])
    for i in range(PARTS):
        write(i).wait()


def swap(x, axes, pairs):
    return lax.ppermute(x, axes, [*pairs, *((b, a) for a, b in pairs)])


def exchange(ex, ox, ey, oy, z):
    evens = [(2 * i, 2 * i + 1) for i in range(8)]
    odds = [(2 * i + 1, (2 * i + 2) % 16) for i in range(8)]
    zr = swap(z, "gz", [(0, 1)])
    return (
        swap(ex, GX, evens),
        swap(ox, GX, odds),
        swap(ey, "gy", [(0, 1), (2, 3)]),
        swap(oy, "gy", [(1, 2), (3, 0)]),
        zr,
    )


VM = pl.BlockSpec(memory_space=pltpu.VMEM)
HB = pl.BlockSpec(memory_space=pltpu.HBM)
BLOCK = (NXL, NYL, NZL)
TILED = (NXL, TILES, 8, NZL)
PADDED = (PX, TILES + 4, 8, NZL)
FACE = (2, TILES, 8, NZL)
FACES = (FACE, FACE, (2, NXL, NZL), (2, NXL, NZL), FACE)


def call(kernel, name, args, outs, scratch, aliases=None):
    return pl.pallas_call(
        kernel,
        out_shape=tuple(vmem(s) for s in outs),
        in_specs=[VM] * len(args),
        out_specs=(VM,) * len(outs),
        input_output_aliases=aliases or {},
        scratch_shapes=[vmem(s) for s in scratch],
        compiler_params=pltpu.CompilerParams(vmem_limit_bytes=LIMIT),
        cost_estimate=cost(),
        name=name,
    )(*map(in_vmem, args))


def cost():
    return pl.CostEstimate(flops=20_000_000, bytes_accessed=10_000_000, transcendentals=0)


def across(name, k, faces, prev, dinv):
    exr, oxr, eyr, oyr, zr = exchange(*faces)
    (part,) = call(inside_kernel, name + "_inside", (k, faces[-1], zr), (TILED,), (FACE, TILED, TILED, TILED))
    acc, kn, *rest = call(
        functools.partial(across_kernel, name == "one"),
        name + "_across",
        (part, k, prev, dinv, exr, oxr, eyr, oyr),
        (TILED, PADDED, *FACES, (2, 8, NZL)),
        ((4, NXL, NZL), (NXL, 4, 8, NZL)),
        {0: 0},
    )
    return acc, kn, rest[:-1], rest[-1], oyr


def per_device(load, stiffness, prestress, state_var, normal_a):
    outs = (TILED, TILED, PADDED, *FACES, (1, 8, NZL))
    b, dinv, k0, *faces, sums0 = pl.pallas_call(
        first_kernel,
        out_shape=tuple(vmem(s) for s in outs),
        in_specs=[HB, HB],
        out_specs=(VM,) * len(outs),
        scratch_shapes=[vmem(BLOCK), vmem(BLOCK), pltpu.SemaphoreType.DMA((PARTS,)), pltpu.SemaphoreType.DMA((PARTS,))],
        compiler_params=pltpu.CompilerParams(vmem_limit_bytes=LIMIT),
        cost_estimate=cost(),
        name="start",
    )(in_hbm(load), in_hbm(stiffness))
    e1, k1, faces1, sums1, oyr0 = across("one", k0, faces, b, dinv)
    e2, k2, faces2, sums2, oyr1 = across("two", k1, faces1, e1, dinv)
    taken2 = exchange(*faces2)
    (part,) = call(inside_sum_kernel, "three_inside", (k2, e2), ((8, NZL),), (TILED,))
    row, own, sent = call(
        last_kernel,
        "last",
        (sums0, sums1, sums2, part, *faces2, *taken2, faces[3], oyr0, faces1[3], oyr1),
        ((128, NZL), (3, 16, NZL), (3, 16, NZL)),
        (),
    )
    got = swap(sent, "gy", [(0, 1), (2, 3)])
    rows = lax.all_to_all(row, ALL, 0, 0, tiled=True)
    out, slip = pl.pallas_call(
        final_kernel,
        out_shape=(jax.ShapeDtypeStruct(BLOCK, F32), jax.ShapeDtypeStruct((16, NZL), F32)),
        in_specs=[HB] * 2 + [VM] * 7,
        out_specs=(HB, VM),
        scratch_shapes=[vmem(TILED), vmem(TILED), vmem(BLOCK)] + [pltpu.SemaphoreType.DMA((PARTS,))] * 3,
        compiler_params=pltpu.CompilerParams(vmem_limit_bytes=LIMIT),
        cost_estimate=cost(),
        name="final",
    )(*map(in_hbm, (k0, k2)), *map(in_vmem, (k1, rows, own, got)), prestress, state_var, normal_a)
    return out, slip


def solution(mesh):
    torus = Mesh(
        mesh.devices.reshape(4, 4, mesh.shape["gy"], mesh.shape["gz"]), ("gx_0", "gx_1", "gy", "gz")
    )
    block = P(GX, "gy", "gz")
    fault = P(GX_GY, "gz")
    return jax.shard_map(
        per_device,
        mesh=torus,
        in_specs=(block, block, fault, fault, fault),
        out_specs=(block, fault),
        check_vma=False,
    )
```

```python
import functools

import jax
import jax.numpy as jnp
from jax import lax
from jax.experimental import pallas as pl
from jax.experimental.pallas import tpu as pltpu
from jax.sharding import Mesh
from jax.sharding import PartitionSpec as P

GX = ("gx_0", "gx_1")
GX_GY = ("gx_0", "gx_1", "gy")
ALL = ("gx_0", "gx_1", "gy", "gz")
F32 = jnp.float32

NXL, NYL, NZL = 64, 64, 128
PX = NXL + 4
PARTS = 8
TILES = 8
LIMIT = 9 * 2**20
AHEAD = 8
AT_ONCE = 8


def vmem(shape):
    return pltpu.VMEM(shape, F32)


def in_vmem(x):
    return pltpu.with_memory_space_constraint(x, pltpu.VMEM)


def in_hbm(x):
    return pltpu.with_memory_space_constraint(x, pltpu.HBM)


def place():
    gx = lax.axis_index("gx_0") * lax.axis_size("gx_1") + lax.axis_index("gx_1")
    return gx, lax.axis_index("gy"), lax.axis_index("gz")


def lanes():
    return lax.broadcasted_iota(jnp.int32, (8, NZL), 1)


def pack_z(x, tile, packed):
    shift = (4 * x + 2) & (NZL - 1)
    return jnp.where(lanes() // 4 == (x & 31), pltpu.roll(tile, shift, 1), packed)


def finish_plane(kn, x, packed):
    sub = lax.broadcasted_iota(jnp.int32, (8, NZL), 0)
    tiles = [kn[x + 2, v + 2] for v in range(TILES)]
    for i in range(2):
        kn[x + 2, i] = jnp.where(sub == 0, 0.0, pltpu.roll(tiles[6 + i], 1, 0))
        kn[x + 2, 10 + i] = jnp.where(sub == 7, 0.0, pltpu.roll(tiles[i], 7, 0))
    return tuple(pack_z(x, t, p) for t, p in zip(tiles, packed))


def zeros(n):
    return tuple(jnp.zeros((8, NZL), F32) for _ in range(n))


class Total:
    def __init__(self):
        self.chains = [None] * 4
        self.count = 0

    def add(self, term):
        at = self.count % 4
        self.chains[at] = term if self.chains[at] is None else self.chains[at] + term
        self.count += 1

    def value(self):
        a, b, c, d = self.chains
        return (a + b) + (c + d)


def clear_sides(kp):
    for x in (0, NXL + 2):
        kp[x : x + 2, 2:10] = jnp.zeros(FACE, F32)


def send_faces(kp, ex, ox, ey, oy):
    gx, gy, _ = place()
    even = lax.rem(gx, 2) == 0

    def planes(up, down):
        up[...] = kp[NXL : NXL + 2, 2:10]
        down[...] = kp[2:4, 2:10]

    @pl.when(even)
    def _():
        planes(ex, ox)

    @pl.when(jnp.logical_not(even))
    def _():
        planes(ox, ex)

    def rows(up, down):
        for x in range(NXL):
            for k in range(2):
                up[k, x : x + 1, :] = kp[x + 2, 8 + k, 7:8, :]
                down[k, x : x + 1, :] = kp[x + 2, 2 + k, 0:1, :]

    even_y = lax.rem(gy, 2) == 0

    @pl.when(even_y)
    def _():
        rows(ey, oy)

    @pl.when(jnp.logical_not(even_y))
    def _():
        rows(oy, ey)


def sides(e, o, at, last):
    even = lax.rem(at, 2) == 0
    return jnp.where(even, o, e), jnp.where(even, e, o)


def taken(e, o, at, last):
    inner = jnp.logical_and(at != 0, at != last)
    return sides(e, jnp.where(inner, o, 0.0), at, last)


def over(low, high):
    return 16.0 * low[1] - low[0], -low[1], -high[0], 16.0 * high[0] - high[1]


def z_terms(terms, z, zr):
    gz = lax.axis_index("gz")
    at = lax.rem(lanes(), 4)
    ours = (at >= 2) == (gz == 0)
    for h in range(2):
        for v in range(TILES):
            d = jnp.where(ours, zr[h, v], 0.0) - z[h, v]
            two = jnp.where(at < 2, pltpu.roll(d, NZL - 2, 1), pltpu.roll(d, 2, 1))
            one = jnp.where(at == 1, pltpu.roll(d, NZL - 1, 1), jnp.where(at == 2, pltpu.roll(d, 1, 1), 0.0))
            terms[h, v] = 16.0 * one - two


def stencil(kp, x, zpart):
    p = [kp[x + 2, j] for j in range(TILES + 4)]
    for v in range(TILES):
        near = (kp[x + 1, v + 2] + kp[x + 3, v + 2]) + (p[v + 1] + p[v + 3])
        far = (kp[x, v + 2] + kp[x + 4, v + 2]) + (p[v] + p[v + 4])
        yield v, (16.0 * near - far) + zpart[x, v]


def inside_kernel(kp, zo, zr, out, terms, one, three, zpart):
    z_terms(terms, zo, zr)
    lane = lanes()
    edge = jnp.logical_or(lane < 2, lane >= NZL - 2)

    def shift_one(x, _):
        return one, x, [pltpu.roll(kp[x + 2, v + 2], 1, 1) for v in range(TILES)]

    def shift_three(x, _):
        return three, x, [pltpu.roll(16.0 * kp[x + 2, v + 2] - one[x, v], 3, 1) for v in range(TILES)]

    def shift_back(x, half):
        back = (126 - 4 * x) & (NZL - 1)
        new = []
        for v in range(TILES):
            w = (16.0 * one[x, v] - kp[x + 2, v + 2]) + three[x, v]
            side = jnp.where(edge, pltpu.roll(terms[half, v], back, 1), 0.0)
            new.append(pltpu.roll(w, NZL - 2, 1) + side)
        return zpart, x, new

    def begin(i, stages):
        begun = []
        for stage, steps in stages:
            half = lax.shift_right_logical(jnp.int32(i + steps), (32 // AHEAD).bit_length() - 1)
            begun += [stage(AHEAD * (i + steps) + x, half) for x in range(AHEAD)]
        return begun

    def end(begun):
        for ref, x, new in begun:
            for v in range(TILES):
                ref[x, v] = new[v]

    for i in range(3):
        end(begin(i, ((shift_one, 0),)))
    for i in range(2):
        end(begin(i, ((shift_three, 0),)))
    end(begin(0, ((shift_back, 0),)))

    stages = ((shift_back, 1), (shift_three, 2), (shift_one, 3))
    steps = NXL // AHEAD

    def planes(i, carry, stages=stages):
        begun = begin(i, stages)
        for x in range(AHEAD):
            x = AHEAD * i + x
            for v, a in list(stencil(kp, x, zpart)):
                out[x, v] = a
        end(begun)
        return carry

    lax.fori_loop(0, steps - 3, planes, 0)
    for i in (steps - 3, steps - 2, steps - 1):
        planes(i, 0, tuple(s for s in stages if i + s[1] < steps))


def inside_sum_kernel(kp, prev, out, zpart):
    def shift(x):
        here = [kp[x + 2, v + 2] for v in range(TILES)]
        return x, [16.0 * pltpu.roll(h, NZL - 1, 1) - pltpu.roll(h, NZL - 2, 1) for h in here]

    def end(begun):
        for x, new in begun:
            for v in range(TILES):
                zpart[x, v] = new[v]

    end([shift(x) for x in range(AHEAD)])

    steps = NXL // AHEAD

    def planes(i, total, ahead=True):
        begun = [shift(AHEAD * (i + 1) + x) for x in range(AHEAD if ahead else 0)]
        parts = Total()
        for x in [AHEAD * i + x for x in range(AHEAD)]:
            p = [kp[x + 2, j] for j in range(2, TILES + 4)]
            for v in range(TILES):
                near = kp[x + 3, v + 2] + p[v + 1]
                far = kp[x + 4, v + 2] + p[v + 2]
                a = (16.0 * near - far) + zpart[x, v]
                parts.add(p[v] * (prev[x, v] - 2.0 * a))
        end(begun)
        return total + parts.value()

    out[...] = planes(steps - 1, lax.fori_loop(0, steps - 1, planes, zeros(1)[0]), False)


def z_pairs(z, zr):
    gz = lax.axis_index("gz")
    at = lax.rem(lanes(), 4)
    parts = Total()
    for h in range(2):
        for v in range(TILES):
            own, other = z[h, v], zr[h, v]
            up = 2.0 * own - jnp.where(gz == 0, other, 0.0)
            down = jnp.where(gz == 0, 0.0, -other)
            up = jnp.where(at == 1, 16.0 * pltpu.roll(up, NZL - 1, 1), 0.0) - pltpu.roll(up, NZL - 2, 1)
            down = jnp.where(at == 2, 16.0 * pltpu.roll(down, 1, 1), 0.0) - pltpu.roll(down, 2, 1)
            parts.add(own * jnp.where(at < 2, up, down))
    return parts.value()


def first_kernel(load, stiff, b, dinv, kp, ex, ox, ey, oy, z, sums, raw, s, sem_b, sem_s):
    step = NXL // PARTS

    def copies(i):
        at = pl.ds(i * step, step)
        return (
            pltpu.make_async_copy(load.at[at], raw.at[at], sem_b.at[i]),
            pltpu.make_async_copy(stiff.at[at], s.at[at], sem_s.at[i]),
        )

    for i in range(PARTS):
        for c in copies(i):
            c.start()
    clear_sides(kp)

    def planes(i, carry):
        packed, total = carry
        for x in range(AT_ONCE):
            packed = finish_plane(kp, AT_ONCE * jnp.maximum(i - 1, 0) + x, packed)
        parts = Total()
        for x in [AT_ONCE * i + x for x in range(AT_ONCE)]:
            for v in range(TILES):
                row = pl.ds(v, 8, stride=TILES)
                inverse = 1.0 / (90.0 + 12.0 * s[x, row, :])
                right = 12.0 * raw[x, row, :]
                k = right * inverse
                b[x, v] = right
                dinv[x, v] = inverse
                kp[x + 2, v + 2] = k
                parts.add(k * right)
        return packed, total + parts.value()

    (total,) = zeros(1)
    packed = zeros(TILES)
    for i in range(PARTS):
        for c in copies(i):
            c.wait()
        packed, total = lax.fori_loop(i * step // AT_ONCE, (i + 1) * step // AT_ONCE, planes, (packed, total))
        if (i + 1) * step % 32 == 0:
            for x in range(AT_ONCE):
                packed = finish_plane(kp, (i + 1) * step - AT_ONCE + x, packed)
            for v in range(TILES):
                z[(i + 1) * step // 32 - 1, v] = packed[v]
    sums[0] = total
    send_faces(kp, ex, ox, ey, oy)


def across_kernel(
    first, part, kp, prev, dinv, exr, oxr, eyr, oyr, acc, kn, ex, ox, ey, oy, z, sums, rows, tiles
):
    del part
    gx, gy, _ = place()
    sub = lax.broadcasted_iota(jnp.int32, (8, NZL), 0)
    clear_sides(kn)
    for x, extra in zip((0, 1, NXL - 2, NXL - 1), over(*taken(exr[...], oxr[...], gx, 15))):
        acc[x] = acc[x] + extra
    for j, extra in enumerate(over(*taken(eyr[...], oyr[...], gy, 3))):
        rows[j] = extra
    for x in range(NXL):
        for j in range(4):
            tiles[x, j] = jnp.where(sub == (0 if j < 2 else 7), rows[j, x : x + 1, :], 0.0)

    def planes(i, carry):
        packed, s0, s1 = carry
        for x in range(AT_ONCE):
            packed = finish_plane(kn, AT_ONCE * jnp.maximum(i - 1, 0) + x, packed)
        p0, p1 = Total(), Total()
        for x in [AT_ONCE * i + x for x in range(AT_ONCE)]:
            for v in range(TILES):
                a = acc[x, v]
                if v in (0, 1, 6, 7):
                    a = a + tiles[x, v if v < 2 else v - 4]
                change = prev[x, v] - a
                new = change if first else a
                k = new * dinv[x, v]
                acc[x, v] = new
                kn[x + 2, v + 2] = k
                p0.add(kp[x + 2, v + 2] * change)
                p1.add(k * change)
        return packed, s0 + p0.value(), s1 + p1.value()

    carry = (zeros(TILES), *zeros(2))
    for h in range(2):
        steps = 32 // AT_ONCE
        packed, s0, s1 = lax.fori_loop(steps * h, steps * h + steps, planes, carry)
        for x in range(AT_ONCE):
            packed = finish_plane(kn, 32 * h + 32 - AT_ONCE + x, packed)
        for v in range(TILES):
            z[h, v] = packed[v]
        carry = (packed, s0, s1)
    sums[0] = s0
    sums[1] = s1
    send_faces(kn, ex, ox, ey, oy)


def last_kernel(*refs):
    sums0, sums1, sums2, part = refs[:4]
    ex, ox, ey, oy, z, exr, oxr, eyr, oyr, zr = refs[4:14]
    pairs = (refs[14:16], refs[16:18], (oy, oyr))
    row, own, sent = refs[18:]
    gx, gy, _ = place()
    m4 = part[...] + z_pairs(z, zr)
    for e, o, er, orr, at, last in ((ex, ox, exr, oxr, gx, 15), (ey, oy, eyr, oyr, gy, 3)):
        low, high = sides(e[...], o[...], at, last)
        extra = over(*taken(er[...], orr[...], at, last))
        gain = low[0] * extra[0] + low[1] * extra[1] + high[0] * extra[2] + high[1] * extra[3]
        m4 = m4 - gain.reshape(8, 8, NZL).sum(axis=0)
    parts = (sums0[0], sums1[0], sums1[1], sums2[0], sums2[1], m4)
    lane = lanes()
    sub = lax.broadcasted_iota(jnp.int32, (8, NZL), 0)
    stack = jnp.zeros((8, NZL), F32)
    for i, p in enumerate(parts):
        stack = jnp.where(sub == i, jnp.sum(p, axis=0, keepdims=True), stack)
    whole = jnp.sum(stack, axis=1, keepdims=True)
    out = jnp.sum(jnp.where(lane == sub, whole, 0.0), axis=0, keepdims=True)
    row[...] = jnp.broadcast_to(out, (128, NZL))
    below = gy == 1
    for j, (mine, other) in enumerate(pairs):
        mine, other = mine[...], other[...]
        a = jnp.where(below, mine, other)
        b = jnp.where(below, other, mine)
        t = (a[0] - b[1] + 27.0 * (b[0] - a[1])) * (1.0 / 24.0)
        sent[j] = jnp.where(below, t[0:16], t[48:64])
        own[j] = jnp.where(below, t[16:32], t[32:48])


def coefficients(rows):
    tot = jnp.sum(rows, axis=0, keepdims=True)
    lane = lax.broadcasted_iota(jnp.int32, (1, NZL), 1)
    v = [jnp.sum(jnp.where(lane == i, tot, 0.0), axis=1, keepdims=True) for i in range(6)]
    v0, g00, g01, g11, g12, g22 = v
    g02 = g01 - g11
    l1 = g01 / g00
    l2 = g02 / g00
    d1 = g11 - l1 * g01
    e = g12 - l2 * g01
    f1 = g00 - l1 * v0
    l3 = e / d1
    d2 = (g22 - l2 * g02) - l3 * e
    f2 = ((g00 - g01) - l2 * v0) - l3 * f1
    c2 = f2 / d2
    c1 = (f1 - e * c2) / d1
    c0 = (v0 - g01 * c1 - g02 * c2) / g00
    return c0, c1, c2


def scaled_sinh(a, s):
    half = 0.6931471805599453
    large = jnp.exp(a - s - half) - jnp.exp(-a - s - half)
    q = a * a
    small = a * (1.0 + q * (1.0 / 6.0 + q * (1.0 / 120.0 + q * (1.0 / 5040.0)))) * jnp.exp(-s)
    return jnp.where(jnp.abs(a) < 0.5, small, large)


def final_kernel(
    k0, k2, k1, rows, own, got, prestress, state, normal, out, slip, r0, r2, buf, sem0, sem2, sem
):
    gy = lax.axis_index("gy")
    step = NXL // PARTS

    def reads(i):
        at = pl.ds(2 + i * step, step)
        to = pl.ds(i * step, step)
        return (
            pltpu.make_async_copy(k0.at[at, pl.ds(2, TILES)], r0.at[to], sem0.at[i]),
            pltpu.make_async_copy(k2.at[at, pl.ds(2, TILES)], r2.at[to], sem2.at[i]),
        )

    def write(i):
        at = pl.ds(i * step, step)
        return pltpu.make_async_copy(buf.at[at], out.at[at], sem.at[i])

    for i in range(PARTS):
        for c in reads(i):
            c.start()
    c0, c1, c2 = coefficients(rows[...])

    def plane(x, carry):
        for v in range(TILES):
            at = pl.ds(v, 8, stride=TILES)
            buf[x, at, :] = c0 * r0[x, v] + c1 * k1[x + 2, v + 2] + c2 * r2[x, v]
        return carry

    for i in range(PARTS):
        for c in reads(i):
            c.wait()
        lax.fori_loop(i * step, (i + 1) * step, plane, 0)
        write(i).start()
    mine = jnp.logical_or(gy == 1, gy == 2)
    t = jnp.where(mine, own[...], got[...])
    traction = c0 * t[0] + c1 * t[1] + c2 * t[2]
    arg = (prestress[...] + 2.0 * traction) / normal[...]
    slip[...] = scaled_sinh(arg, state[...])
    for i in range(PARTS):
        write(i).wait()


def swap(x, axes, pairs):
    return lax.ppermute(x, axes, [*pairs, *((b, a) for a, b in pairs)])


def odd_pairs(along):
    pairs = []
    for gx in range(16):
        for gy in range(4):
            for gz in range(2):
                at, count = (gx, 16) if along == "gx" else (gy, 4)
                here = (gx * 4 + gy) * 2 + gz
                step = 8 if along == "gx" else 2
                if at % 2 == 1 and at < count - 1:
                    pairs.append((here, here + step))
                elif at in (0, count - 1) and gz == 0:
                    pairs.append((here, here + 1))
    return pairs


def exchange(ex, ox, ey, oy, z):
    evens = [(2 * i, 2 * i + 1) for i in range(8)]
    zr = swap(z, "gz", [(0, 1)])
    return (
        swap(ex, GX, evens),
        swap(ox, ALL, odd_pairs("gx")),
        swap(ey, "gy", [(0, 1), (2, 3)]),
        swap(oy, ALL, odd_pairs("gy")),
        zr,
    )


VM = pl.BlockSpec(memory_space=pltpu.VMEM)
HB = pl.BlockSpec(memory_space=pltpu.HBM)
BLOCK = (NXL, NYL, NZL)
TILED = (NXL, TILES, 8, NZL)
PADDED = (PX, TILES + 4, 8, NZL)
FACE = (2, TILES, 8, NZL)
FACES = (FACE, FACE, (2, NXL, NZL), (2, NXL, NZL), FACE)


def call(kernel, name, args, outs, scratch, aliases=None):
    return pl.pallas_call(
        kernel,
        out_shape=tuple(vmem(s) for s in outs),
        in_specs=[VM] * len(args),
        out_specs=(VM,) * len(outs),
        input_output_aliases=aliases or {},
        scratch_shapes=[vmem(s) for s in scratch],
        compiler_params=pltpu.CompilerParams(vmem_limit_bytes=LIMIT),
        cost_estimate=cost(),
        name=name,
    )(*map(in_vmem, args))


def cost():
    return pl.CostEstimate(flops=20_000_000, bytes_accessed=10_000_000, transcendentals=0)


def across(name, k, faces, prev, dinv):
    exr, oxr, eyr, oyr, zr = exchange(*faces)
    (part,) = call(inside_kernel, name + "_inside", (k, faces[-1], zr), (TILED,), (FACE, TILED, TILED, TILED))
    acc, kn, *rest = call(
        functools.partial(across_kernel, name == "one"),
        name + "_across",
        (part, k, prev, dinv, exr, oxr, eyr, oyr),
        (TILED, PADDED, *FACES, (2, 8, NZL)),
        ((4, NXL, NZL), (NXL, 4, 8, NZL)),
        {0: 0},
    )
    return acc, kn, rest[:-1], rest[-1], oyr


def per_device(load, stiffness, prestress, state_var, normal_a):
    outs = (TILED, TILED, PADDED, *FACES, (1, 8, NZL))
    b, dinv, k0, *faces, sums0 = pl.pallas_call(
        first_kernel,
        out_shape=tuple(vmem(s) for s in outs),
        in_specs=[HB, HB],
        out_specs=(VM,) * len(outs),
        scratch_shapes=[vmem(BLOCK), vmem(BLOCK), pltpu.SemaphoreType.DMA((PARTS,)), pltpu.SemaphoreType.DMA((PARTS,))],
        compiler_params=pltpu.CompilerParams(vmem_limit_bytes=LIMIT),
        cost_estimate=cost(),
        name="start",
    )(in_hbm(load), in_hbm(stiffness))
    e1, k1, faces1, sums1, oyr0 = across("one", k0, faces, b, dinv)
    e2, k2, faces2, sums2, oyr1 = across("two", k1, faces1, e1, dinv)
    taken2 = exchange(*faces2)
    (part,) = call(inside_sum_kernel, "three_inside", (k2, e2), ((8, NZL),), (TILED,))
    row, own, sent = call(
        last_kernel,
        "last",
        (sums0, sums1, sums2, part, *faces2, *taken2, faces[3], oyr0, faces1[3], oyr1),
        ((128, NZL), (3, 16, NZL), (3, 16, NZL)),
        (),
    )
    got = swap(sent, "gy", [(0, 1), (2, 3)])
    rows = lax.all_to_all(row, ALL, 0, 0, tiled=True)
    out, slip = pl.pallas_call(
        final_kernel,
        out_shape=(jax.ShapeDtypeStruct(BLOCK, F32), jax.ShapeDtypeStruct((16, NZL), F32)),
        in_specs=[HB] * 2 + [VM] * 7,
        out_specs=(HB, VM),
        scratch_shapes=[vmem(TILED), vmem(TILED), vmem(BLOCK)] + [pltpu.SemaphoreType.DMA((PARTS,))] * 3,
        compiler_params=pltpu.CompilerParams(vmem_limit_bytes=LIMIT),
        cost_estimate=cost(),
        name="final",
    )(*map(in_hbm, (k0, k2)), *map(in_vmem, (k1, rows, own, got)), prestress, state_var, normal_a)
    return out, slip


def solution(mesh):
    torus = Mesh(
        mesh.devices.reshape(4, 4, mesh.shape["gy"], mesh.shape["gz"]), ("gx_0", "gx_1", "gy", "gz")
    )
    block = P(GX, "gy", "gz")
    fault = P(GX_GY, "gz")
    return jax.shard_map(
        per_device,
        mesh=torus,
        in_specs=(block, block, fault, fault, fault),
        out_specs=(block, fault),
        check_vma=False,
    )
```

```python
import functools

import jax
import jax.numpy as jnp
from jax import lax
from jax.experimental import pallas as pl
from jax.experimental.pallas import tpu as pltpu
from jax.sharding import Mesh
from jax.sharding import PartitionSpec as P

GX = ("gx_0", "gx_1")
GX_GY = ("gx_0", "gx_1", "gy")
ALL = ("gx_0", "gx_1", "gy", "gz")
F32 = jnp.float32

NXL, NYL, NZL = 64, 64, 128
PX = NXL + 4
PARTS = 8
TILES = 8
LIMIT = 9 * 2**20
AHEAD = 8
AT_ONCE = 8


def vmem(shape):
    return pltpu.VMEM(shape, F32)


def in_vmem(x):
    return pltpu.with_memory_space_constraint(x, pltpu.VMEM)


def in_hbm(x):
    return pltpu.with_memory_space_constraint(x, pltpu.HBM)


def place():
    gx = lax.axis_index("gx_0") * lax.axis_size("gx_1") + lax.axis_index("gx_1")
    return gx, lax.axis_index("gy"), lax.axis_index("gz")


def lanes():
    return lax.broadcasted_iota(jnp.int32, (8, NZL), 1)


def pack_z(x, tile, packed):
    shift = (4 * x + 2) & (NZL - 1)
    return jnp.where(lanes() // 4 == (x & 31), pltpu.roll(tile, shift, 1), packed)


def finish_plane(kn, x, packed):
    sub = lax.broadcasted_iota(jnp.int32, (8, NZL), 0)
    tiles = [kn[x + 2, v + 2] for v in range(TILES)]
    for i in range(2):
        kn[x + 2, i] = jnp.where(sub == 0, 0.0, pltpu.roll(tiles[6 + i], 1, 0))
        kn[x + 2, 10 + i] = jnp.where(sub == 7, 0.0, pltpu.roll(tiles[i], 7, 0))
    return tuple(pack_z(x, t, p) for t, p in zip(tiles, packed))


def zeros(n):
    return tuple(jnp.zeros((8, NZL), F32) for _ in range(n))


class Total:
    def __init__(self):
        self.chains = [None] * 4
        self.count = 0

    def add(self, term):
        at = self.count % 4
        self.chains[at] = term if self.chains[at] is None else self.chains[at] + term
        self.count += 1

    def value(self):
        a, b, c, d = self.chains
        return (a + b) + (c + d)


def clear_sides(kp):
    for x in (0, NXL + 2):
        kp[x : x + 2, 2:10] = jnp.zeros(FACE, F32)


def send_faces(kp, ex, ox, ey, oy):
    gx, gy, _ = place()
    even = lax.rem(gx, 2) == 0

    def planes(up, down):
        up[...] = kp[NXL : NXL + 2, 2:10]
        down[...] = kp[2:4, 2:10]

    @pl.when(even)
    def _():
        planes(ex, ox)

    @pl.when(jnp.logical_not(even))
    def _():
        planes(ox, ex)

    def rows(up, down):
        for x in range(NXL):
            for k in range(2):
                up[k, x : x + 1, :] = kp[x + 2, 8 + k, 7:8, :]
                down[k, x : x + 1, :] = kp[x + 2, 2 + k, 0:1, :]

    even_y = lax.rem(gy, 2) == 0

    @pl.when(even_y)
    def _():
        rows(ey, oy)

    @pl.when(jnp.logical_not(even_y))
    def _():
        rows(oy, ey)


def sides(e, o, at, last):
    even = lax.rem(at, 2) == 0
    return jnp.where(even, o, e), jnp.where(even, e, o)


def taken(e, o, at, last):
    inner = jnp.logical_and(at != 0, at != last)
    return sides(e, jnp.where(inner, o, 0.0), at, last)


def over(low, high):
    return 16.0 * low[1] - low[0], -low[1], -high[0], 16.0 * high[0] - high[1]


def z_terms(terms, z, zr):
    gz = lax.axis_index("gz")
    at = lax.rem(lanes(), 4)
    ours = (at >= 2) == (gz == 0)
    for h in range(2):
        for v in range(TILES):
            d = jnp.where(ours, zr[h, v], 0.0) - z[h, v]
            two = jnp.where(at < 2, pltpu.roll(d, NZL - 2, 1), pltpu.roll(d, 2, 1))
            one = jnp.where(at == 1, pltpu.roll(d, NZL - 1, 1), jnp.where(at == 2, pltpu.roll(d, 1, 1), 0.0))
            terms[h, v] = 16.0 * one - two


def stencil(kp, x, zpart):
    p = [kp[x + 2, j] for j in range(TILES + 4)]
    for v in range(TILES):
        near = (kp[x + 1, v + 2] + kp[x + 3, v + 2]) + (p[v + 1] + p[v + 3])
        far = (kp[x, v + 2] + kp[x + 4, v + 2]) + (p[v] + p[v + 4])
        yield v, (16.0 * near - far) + zpart[x, v]


def inside_kernel(kp, zo, zr, out, terms, one, three, zpart):
    z_terms(terms, zo, zr)
    lane = lanes()
    edge = jnp.logical_or(lane < 2, lane >= NZL - 2)

    def shift_one(x, _):
        return one, x, [pltpu.roll(kp[x + 2, v + 2], 1, 1) for v in range(TILES)]

    def shift_three(x, _):
        return three, x, [pltpu.roll(16.0 * kp[x + 2, v + 2] - one[x, v], 3, 1) for v in range(TILES)]

    def shift_back(x, half):
        back = (126 - 4 * x) & (NZL - 1)
        new = []
        for v in range(TILES):
            w = (16.0 * one[x, v] - kp[x + 2, v + 2]) + three[x, v]
            side = jnp.where(edge, pltpu.roll(terms[half, v], back, 1), 0.0)
            new.append(pltpu.roll(w, NZL - 2, 1) + side)
        return zpart, x, new

    def begin(i, stages):
        begun = []
        for stage, steps in stages:
            half = AHEAD * (i + steps) // 32
            begun += [stage(AHEAD * (i + steps) + x, half) for x in range(AHEAD)]
        return begun

    def end(begun):
        for ref, x, new in begun:
            for v in range(TILES):
                ref[x, v] = new[v]

    for i in range(3):
        end(begin(i, ((shift_one, 0),)))
    for i in range(2):
        end(begin(i, ((shift_three, 0),)))
    end(begin(0, ((shift_back, 0),)))

    stages = ((shift_back, 1), (shift_three, 2), (shift_one, 3))
    steps = NXL // AHEAD

    def planes(i, carry, stages=stages):
        begun = begin(i, stages)
        for x in range(AHEAD):
            x = AHEAD * i + x
            for v, a in list(stencil(kp, x, zpart)):
                out[x, v] = a
        end(begun)
        return carry

    for i in range(steps):
        planes(i, 0, tuple(s for s in stages if i + s[1] < steps))


def inside_sum_kernel(kp, prev, out, zpart):
    def shift(x):
        here = [kp[x + 2, v + 2] for v in range(TILES)]
        return x, [16.0 * pltpu.roll(h, NZL - 1, 1) - pltpu.roll(h, NZL - 2, 1) for h in here]

    def end(begun):
        for x, new in begun:
            for v in range(TILES):
                zpart[x, v] = new[v]

    end([shift(x) for x in range(AHEAD)])

    steps = NXL // AHEAD

    def planes(i, total, ahead=True):
        begun = [shift(AHEAD * (i + 1) + x) for x in range(AHEAD if ahead else 0)]
        parts = Total()
        for x in [AHEAD * i + x for x in range(AHEAD)]:
            p = [kp[x + 2, j] for j in range(2, TILES + 4)]
            for v in range(TILES):
                near = kp[x + 3, v + 2] + p[v + 1]
                far = kp[x + 4, v + 2] + p[v + 2]
                a = (16.0 * near - far) + zpart[x, v]
                parts.add(p[v] * (prev[x, v] - 2.0 * a))
        end(begun)
        return total + parts.value()

    (total,) = zeros(1)
    for i in range(steps):
        total = planes(i, total, i + 1 < steps)
    out[...] = total


def z_pairs(z, zr):
    gz = lax.axis_index("gz")
    at = lax.rem(lanes(), 4)
    parts = Total()
    for h in range(2):
        for v in range(TILES):
            own, other = z[h, v], zr[h, v]
            up = 2.0 * own - jnp.where(gz == 0, other, 0.0)
            down = jnp.where(gz == 0, 0.0, -other)
            up = jnp.where(at == 1, 16.0 * pltpu.roll(up, NZL - 1, 1), 0.0) - pltpu.roll(up, NZL - 2, 1)
            down = jnp.where(at == 2, 16.0 * pltpu.roll(down, 1, 1), 0.0) - pltpu.roll(down, 2, 1)
            parts.add(own * jnp.where(at < 2, up, down))
    return parts.value()


def first_kernel(load, stiff, b, dinv, kp, ex, ox, ey, oy, z, sums, raw, s, sem_b, sem_s):
    step = NXL // PARTS

    def copies(i):
        at = pl.ds(i * step, step)
        return (
            pltpu.make_async_copy(load.at[at], raw.at[at], sem_b.at[i]),
            pltpu.make_async_copy(stiff.at[at], s.at[at], sem_s.at[i]),
        )

    for i in range(PARTS):
        for c in copies(i):
            c.start()
    clear_sides(kp)

    def planes(i, carry):
        packed, total = carry
        for x in range(AT_ONCE):
            packed = finish_plane(kp, AT_ONCE * jnp.maximum(i - 1, 0) + x, packed)
        parts = Total()
        for x in [AT_ONCE * i + x for x in range(AT_ONCE)]:
            for v in range(TILES):
                row = pl.ds(v, 8, stride=TILES)
                inverse = 1.0 / (90.0 + 12.0 * s[x, row, :])
                right = 12.0 * raw[x, row, :]
                k = right * inverse
                b[x, v] = right
                dinv[x, v] = inverse
                kp[x + 2, v + 2] = k
                parts.add(k * right)
        return packed, total + parts.value()

    (total,) = zeros(1)
    packed = zeros(TILES)
    for i in range(PARTS):
        for c in copies(i):
            c.wait()
        packed, total = lax.fori_loop(i * step // AT_ONCE, (i + 1) * step // AT_ONCE, planes, (packed, total))
        if (i + 1) * step % 32 == 0:
            for x in range(AT_ONCE):
                packed = finish_plane(kp, (i + 1) * step - AT_ONCE + x, packed)
            for v in range(TILES):
                z[(i + 1) * step // 32 - 1, v] = packed[v]
    sums[0] = total
    send_faces(kp, ex, ox, ey, oy)


def across_kernel(
    first, part, kp, prev, dinv, exr, oxr, eyr, oyr, acc, kn, ex, ox, ey, oy, z, sums, rows, tiles
):
    del part
    gx, gy, _ = place()
    sub = lax.broadcasted_iota(jnp.int32, (8, NZL), 0)
    clear_sides(kn)
    for x, extra in zip((0, 1, NXL - 2, NXL - 1), over(*taken(exr[...], oxr[...], gx, 15))):
        acc[x] = acc[x] + extra
    for j, extra in enumerate(over(*taken(eyr[...], oyr[...], gy, 3))):
        rows[j] = extra
    for x in range(NXL):
        for j in range(4):
            tiles[x, j] = jnp.where(sub == (0 if j < 2 else 7), rows[j, x : x + 1, :], 0.0)

    packed = zeros(TILES)
    s0, s1 = zeros(2)
    for i in range(NXL // AT_ONCE + 1):
        for x in range(AT_ONCE if i else 0):
            packed = finish_plane(kn, AT_ONCE * (i - 1) + x, packed)
        if AT_ONCE * i in (NXL // 2, NXL):
            for v in range(TILES):
                z[AT_ONCE * i // (NXL // 2) - 1, v] = packed[v]
        if AT_ONCE * i == NXL:
            break
        p0, p1 = Total(), Total()
        for x in [AT_ONCE * i + x for x in range(AT_ONCE)]:
            for v in range(TILES):
                a = acc[x, v]
                if v in (0, 1, 6, 7):
                    a = a + tiles[x, v if v < 2 else v - 4]
                change = prev[x, v] - a
                new = change if first else a
                k = new * dinv[x, v]
                acc[x, v] = new
                kn[x + 2, v + 2] = k
                p0.add(kp[x + 2, v + 2] * change)
                p1.add(k * change)
        s0 = s0 + p0.value()
        s1 = s1 + p1.value()
    sums[0] = s0
    sums[1] = s1
    send_faces(kn, ex, ox, ey, oy)


def last_kernel(*refs):
    sums0, sums1, sums2, part = refs[:4]
    ex, ox, ey, oy, z, exr, oxr, eyr, oyr, zr = refs[4:14]
    pairs = (refs[14:16], refs[16:18], (oy, oyr))
    row, own, sent = refs[18:]
    gx, gy, _ = place()
    m4 = part[...] + z_pairs(z, zr)
    for e, o, er, orr, at, last in ((ex, ox, exr, oxr, gx, 15), (ey, oy, eyr, oyr, gy, 3)):
        low, high = sides(e[...], o[...], at, last)
        extra = over(*taken(er[...], orr[...], at, last))
        gain = low[0] * extra[0] + low[1] * extra[1] + high[0] * extra[2] + high[1] * extra[3]
        m4 = m4 - gain.reshape(8, 8, NZL).sum(axis=0)
    parts = (sums0[0], sums1[0], sums1[1], sums2[0], sums2[1], m4)
    lane = lanes()
    sub = lax.broadcasted_iota(jnp.int32, (8, NZL), 0)
    stack = jnp.zeros((8, NZL), F32)
    for i, p in enumerate(parts):
        stack = jnp.where(sub == i, jnp.sum(p, axis=0, keepdims=True), stack)
    whole = jnp.sum(stack, axis=1, keepdims=True)
    out = jnp.sum(jnp.where(lane == sub, whole, 0.0), axis=0, keepdims=True)
    row[...] = jnp.broadcast_to(out, (128, NZL))
    below = gy == 1
    for j, (mine, other) in enumerate(pairs):
        mine, other = mine[...], other[...]
        a = jnp.where(below, mine, other)
        b = jnp.where(below, other, mine)
        t = (a[0] - b[1] + 27.0 * (b[0] - a[1])) * (1.0 / 24.0)
        sent[j] = jnp.where(below, t[0:16], t[48:64])
        own[j] = jnp.where(below, t[16:32], t[32:48])


def coefficients(rows):
    tot = jnp.sum(rows, axis=0, keepdims=True)
    lane = lax.broadcasted_iota(jnp.int32, (1, NZL), 1)
    v = [jnp.sum(jnp.where(lane == i, tot, 0.0), axis=1, keepdims=True) for i in range(6)]
    v0, g00, g01, g11, g12, g22 = v
    g02 = g01 - g11
    l1 = g01 / g00
    l2 = g02 / g00
    d1 = g11 - l1 * g01
    e = g12 - l2 * g01
    f1 = g00 - l1 * v0
    l3 = e / d1
    d2 = (g22 - l2 * g02) - l3 * e
    f2 = ((g00 - g01) - l2 * v0) - l3 * f1
    c2 = f2 / d2
    c1 = (f1 - e * c2) / d1
    c0 = (v0 - g01 * c1 - g02 * c2) / g00
    return c0, c1, c2


def scaled_sinh(a, s):
    half = 0.6931471805599453
    large = jnp.exp(a - s - half) - jnp.exp(-a - s - half)
    q = a * a
    small = a * (1.0 + q * (1.0 / 6.0 + q * (1.0 / 120.0 + q * (1.0 / 5040.0)))) * jnp.exp(-s)
    return jnp.where(jnp.abs(a) < 0.5, small, large)


def final_kernel(
    k0, k2, k1, rows, own, got, prestress, state, normal, out, slip, r0, r2, buf, sem0, sem2, sem
):
    gy = lax.axis_index("gy")
    step = NXL // PARTS

    def reads(i):
        at = pl.ds(2 + i * step, step)
        to = pl.ds(i * step, step)
        return (
            pltpu.make_async_copy(k0.at[at, pl.ds(2, TILES)], r0.at[to], sem0.at[i]),
            pltpu.make_async_copy(k2.at[at, pl.ds(2, TILES)], r2.at[to], sem2.at[i]),
        )

    def write(i):
        at = pl.ds(i * step, step)
        return pltpu.make_async_copy(buf.at[at], out.at[at], sem.at[i])

    for i in range(PARTS):
        for c in reads(i):
            c.start()
    c0, c1, c2 = coefficients(rows[...])

    def plane(x, carry):
        for v in range(TILES):
            at = pl.ds(v, 8, stride=TILES)
            buf[x, at, :] = c0 * r0[x, v] + c1 * k1[x + 2, v + 2] + c2 * r2[x, v]
        return carry

    for i in range(PARTS):
        for c in reads(i):
            c.wait()
        lax.fori_loop(i * step, (i + 1) * step, plane, 0)
        write(i).start()
    mine = jnp.logical_or(gy == 1, gy == 2)
    t = jnp.where(mine, own[...], got[...])
    traction = c0 * t[0] + c1 * t[1] + c2 * t[2]
    arg = (prestress[...] + 2.0 * traction) / normal[...]
    slip[...] = scaled_sinh(arg, state[...])
    for i in range(PARTS):
        write(i).wait()


def swap(x, axes, pairs):
    return lax.ppermute(x, axes, [*pairs, *((b, a) for a, b in pairs)])


def odd_pairs(along):
    pairs = []
    for gx in range(16):
        for gy in range(4):
            for gz in range(2):
                at, count = (gx, 16) if along == "gx" else (gy, 4)
                here = (gx * 4 + gy) * 2 + gz
                step = 8 if along == "gx" else 2
                if at % 2 == 1 and at < count - 1:
                    pairs.append((here, here + step))
                elif at in (0, count - 1) and gz == 0:
                    pairs.append((here, here + 1))
    return pairs


def exchange(ex, ox, ey, oy, z):
    evens = [(2 * i, 2 * i + 1) for i in range(8)]
    zr = swap(z, "gz", [(0, 1)])
    return (
        swap(ex, GX, evens),
        swap(ox, ALL, odd_pairs("gx")),
        swap(ey, "gy", [(0, 1), (2, 3)]),
        swap(oy, ALL, odd_pairs("gy")),
        zr,
    )


VM = pl.BlockSpec(memory_space=pltpu.VMEM)
HB = pl.BlockSpec(memory_space=pltpu.HBM)
BLOCK = (NXL, NYL, NZL)
TILED = (NXL, TILES, 8, NZL)
PADDED = (PX, TILES + 4, 8, NZL)
FACE = (2, TILES, 8, NZL)
FACES = (FACE, FACE, (2, NXL, NZL), (2, NXL, NZL), FACE)


def call(kernel, name, args, outs, scratch, aliases=None):
    return pl.pallas_call(
        kernel,
        out_shape=tuple(vmem(s) for s in outs),
        in_specs=[VM] * len(args),
        out_specs=(VM,) * len(outs),
        input_output_aliases=aliases or {},
        scratch_shapes=[vmem(s) for s in scratch],
        compiler_params=pltpu.CompilerParams(vmem_limit_bytes=LIMIT),
        cost_estimate=cost(),
        name=name,
    )(*map(in_vmem, args))


def cost():
    return pl.CostEstimate(flops=20_000_000, bytes_accessed=10_000_000, transcendentals=0)


def across(name, k, faces, prev, dinv):
    exr, oxr, eyr, oyr, zr = exchange(*faces)
    (part,) = call(inside_kernel, name + "_inside", (k, faces[-1], zr), (TILED,), (FACE, TILED, TILED, TILED))
    acc, kn, *rest = call(
        functools.partial(across_kernel, name == "one"),
        name + "_across",
        (part, k, prev, dinv, exr, oxr, eyr, oyr),
        (TILED, PADDED, *FACES, (2, 8, NZL)),
        ((4, NXL, NZL), (NXL, 4, 8, NZL)),
        {0: 0},
    )
    return acc, kn, rest[:-1], rest[-1], oyr


def per_device(load, stiffness, prestress, state_var, normal_a):
    outs = (TILED, TILED, PADDED, *FACES, (1, 8, NZL))
    b, dinv, k0, *faces, sums0 = pl.pallas_call(
        first_kernel,
        out_shape=tuple(vmem(s) for s in outs),
        in_specs=[HB, HB],
        out_specs=(VM,) * len(outs),
        scratch_shapes=[vmem(BLOCK), vmem(BLOCK), pltpu.SemaphoreType.DMA((PARTS,)), pltpu.SemaphoreType.DMA((PARTS,))],
        compiler_params=pltpu.CompilerParams(vmem_limit_bytes=LIMIT),
        cost_estimate=cost(),
        name="start",
    )(in_hbm(load), in_hbm(stiffness))
    e1, k1, faces1, sums1, oyr0 = across("one", k0, faces, b, dinv)
    e2, k2, faces2, sums2, oyr1 = across("two", k1, faces1, e1, dinv)
    taken2 = exchange(*faces2)
    (part,) = call(inside_sum_kernel, "three_inside", (k2, e2), ((8, NZL),), (TILED,))
    row, own, sent = call(
        last_kernel,
        "last",
        (sums0, sums1, sums2, part, *faces2, *taken2, faces[3], oyr0, faces1[3], oyr1),
        ((128, NZL), (3, 16, NZL), (3, 16, NZL)),
        (),
    )
    got = swap(sent, "gy", [(0, 1), (2, 3)])
    rows = lax.all_to_all(row, ALL, 0, 0, tiled=True)
    out, slip = pl.pallas_call(
        final_kernel,
        out_shape=(jax.ShapeDtypeStruct(BLOCK, F32), jax.ShapeDtypeStruct((16, NZL), F32)),
        in_specs=[HB] * 2 + [VM] * 7,
        out_specs=(HB, VM),
        scratch_shapes=[vmem(TILED), vmem(TILED), vmem(BLOCK)] + [pltpu.SemaphoreType.DMA((PARTS,))] * 3,
        compiler_params=pltpu.CompilerParams(vmem_limit_bytes=LIMIT),
        cost_estimate=cost(),
        name="final",
    )(*map(in_hbm, (k0, k2)), *map(in_vmem, (k1, rows, own, got)), prestress, state_var, normal_a)
    return out, slip


def solution(mesh):
    torus = Mesh(
        mesh.devices.reshape(4, 4, mesh.shape["gy"], mesh.shape["gz"]), ("gx_0", "gx_1", "gy", "gz")
    )
    block = P(GX, "gy", "gz")
    fault = P(GX_GY, "gz")
    return jax.shard_map(
        per_device,
        mesh=torus,
        in_specs=(block, block, fault, fault, fault),
        out_specs=(block, fault),
        check_vma=False,
    )
```

```python
import functools

import jax
import jax.numpy as jnp
from jax import lax
from jax.experimental import pallas as pl
from jax.experimental.pallas import tpu as pltpu
from jax.sharding import Mesh
from jax.sharding import PartitionSpec as P

GX = ("gx_0", "gx_1")
GX_GY = ("gx_0", "gx_1", "gy")
ALL = ("gx_0", "gx_1", "gy", "gz")
F32 = jnp.float32

NXL, NYL, NZL = 64, 64, 128
PX = NXL + 4
PARTS = 8
TILES = 8
LIMIT = 9 * 2**20
AHEAD = 8
AT_ONCE = 8


def vmem(shape):
    return pltpu.VMEM(shape, F32)


def in_vmem(x):
    return pltpu.with_memory_space_constraint(x, pltpu.VMEM)


def in_hbm(x):
    return pltpu.with_memory_space_constraint(x, pltpu.HBM)


def place():
    gx = lax.axis_index("gx_0") * lax.axis_size("gx_1") + lax.axis_index("gx_1")
    return gx, lax.axis_index("gy"), lax.axis_index("gz")


def lanes():
    return lax.broadcasted_iota(jnp.int32, (8, NZL), 1)


def pack_z(x, tile, packed):
    shift = (4 * x + 2) & (NZL - 1)
    return jnp.where(lanes() // 4 == (x & 31), pltpu.roll(tile, shift, 1), packed)


def finish_plane(kn, x, packed):
    sub = lax.broadcasted_iota(jnp.int32, (8, NZL), 0)
    tiles = [kn[x + 2, v + 2] for v in range(TILES)]
    for i in range(2):
        kn[x + 2, i] = jnp.where(sub == 0, 0.0, pltpu.roll(tiles[6 + i], 1, 0))
        kn[x + 2, 10 + i] = jnp.where(sub == 7, 0.0, pltpu.roll(tiles[i], 7, 0))
    return tuple(pack_z(x, t, p) for t, p in zip(tiles, packed))


def zeros(n):
    return tuple(jnp.zeros((8, NZL), F32) for _ in range(n))


class Total:
    def __init__(self):
        self.chains = [None] * 4
        self.count = 0

    def add(self, term):
        at = self.count % 4
        self.chains[at] = term if self.chains[at] is None else self.chains[at] + term
        self.count += 1

    def value(self):
        a, b, c, d = self.chains
        return (a + b) + (c + d)


def clear_sides(kp):
    for x in (0, NXL + 2):
        kp[x : x + 2, 2:10] = jnp.zeros(FACE, F32)


def send_faces(kp, ex, ox, ey, oy):
    gx, gy, _ = place()
    even = lax.rem(gx, 2) == 0

    def planes(up, down):
        up[...] = kp[NXL : NXL + 2, 2:10]
        down[...] = kp[2:4, 2:10]

    @pl.when(even)
    def _():
        planes(ex, ox)

    @pl.when(jnp.logical_not(even))
    def _():
        planes(ox, ex)

    def rows(up, down):
        for x in range(NXL):
            for k in range(2):
                up[k, x : x + 1, :] = kp[x + 2, 8 + k, 7:8, :]
                down[k, x : x + 1, :] = kp[x + 2, 2 + k, 0:1, :]

    even_y = lax.rem(gy, 2) == 0

    @pl.when(even_y)
    def _():
        rows(ey, oy)

    @pl.when(jnp.logical_not(even_y))
    def _():
        rows(oy, ey)


def sides(e, o, at, last):
    even = lax.rem(at, 2) == 0
    return jnp.where(even, o, e), jnp.where(even, e, o)


def taken(e, o, at, last):
    inner = jnp.logical_and(at != 0, at != last)
    return sides(e, jnp.where(inner, o, 0.0), at, last)


def over(low, high):
    return 16.0 * low[1] - low[0], -low[1], -high[0], 16.0 * high[0] - high[1]


def z_terms(terms, z, zr):
    gz = lax.axis_index("gz")
    at = lax.rem(lanes(), 4)
    ours = (at >= 2) == (gz == 0)
    for h in range(2):
        for v in range(TILES):
            d = jnp.where(ours, zr[h, v], 0.0) - z[h, v]
            two = jnp.where(at < 2, pltpu.roll(d, NZL - 2, 1), pltpu.roll(d, 2, 1))
            one = jnp.where(at == 1, pltpu.roll(d, NZL - 1, 1), jnp.where(at == 2, pltpu.roll(d, 1, 1), 0.0))
            terms[h, v] = 16.0 * one - two


def stencil(kp, x, zpart):
    p = [kp[x + 2, j] for j in range(TILES + 4)]
    for v in range(TILES):
        near = (kp[x + 1, v + 2] + kp[x + 3, v + 2]) + (p[v + 1] + p[v + 3])
        far = (kp[x, v + 2] + kp[x + 4, v + 2]) + (p[v] + p[v + 4])
        yield v, (16.0 * near - far) + zpart[x, v]


def inside_kernel(kp, zo, zr, out, terms, one, three, zpart):
    z_terms(terms, zo, zr)
    lane = lanes()
    edge = jnp.logical_or(lane < 2, lane >= NZL - 2)

    def shift_one(x, _):
        return one, x, [pltpu.roll(kp[x + 2, v + 2], 1, 1) for v in range(TILES)]

    def shift_three(x, _):
        return three, x, [pltpu.roll(16.0 * kp[x + 2, v + 2] - one[x, v], 3, 1) for v in range(TILES)]

    def shift_back(x, half):
        back = (126 - 4 * x) & (NZL - 1)
        new = []
        for v in range(TILES):
            w = (16.0 * one[x, v] - kp[x + 2, v + 2]) + three[x, v]
            side = jnp.where(edge, pltpu.roll(terms[half, v], back, 1), 0.0)
            new.append(pltpu.roll(w, NZL - 2, 1) + side)
        return zpart, x, new

    def begin(i, stages):
        begun = []
        for stage, steps in stages:
            half = AHEAD * (i + steps) // 32
            begun += [stage(AHEAD * (i + steps) + x, half) for x in range(AHEAD)]
        return begun

    def end(begun):
        for ref, x, new in begun:
            for v in range(TILES):
                ref[x, v] = new[v]

    for i in range(3):
        end(begin(i, ((shift_one, 0),)))
    for i in range(2):
        end(begin(i, ((shift_three, 0),)))
    end(begin(0, ((shift_back, 0),)))

    stages = ((shift_back, 1), (shift_three, 2), (shift_one, 3))
    steps = NXL // AHEAD

    def planes(i, carry, stages=stages):
        begun = begin(i, stages)
        for x in range(AHEAD):
            x = AHEAD * i + x
            for v, a in list(stencil(kp, x, zpart)):
                out[x, v] = a
        end(begun)
        return carry

    for i in range(steps):
        planes(i, 0, tuple(s for s in stages if i + s[1] < steps))


def inside_sum_kernel(kp, prev, z, zr, out, zpart):
    def shift(x):
        here = [kp[x + 2, v + 2] for v in range(TILES)]
        return x, [16.0 * pltpu.roll(h, NZL - 1, 1) - pltpu.roll(h, NZL - 2, 1) for h in here]

    def end(begun):
        for x, new in begun:
            for v in range(TILES):
                zpart[x, v] = new[v]

    end([shift(x) for x in range(AHEAD)])

    steps = NXL // AHEAD

    def planes(i, total, ahead=True):
        begun = [shift(AHEAD * (i + 1) + x) for x in range(AHEAD if ahead else 0)]
        parts = Total()
        for x in [AHEAD * i + x for x in range(AHEAD)]:
            p = [kp[x + 2, j] for j in range(2, TILES + 4)]
            for v in range(TILES):
                near = kp[x + 3, v + 2] + p[v + 1]
                far = kp[x + 4, v + 2] + p[v + 2]
                a = (16.0 * near - far) + zpart[x, v]
                parts.add(p[v] * (prev[x, v] - 2.0 * a))
        end(begun)
        return total + parts.value()

    (total,) = zeros(1)
    for i in range(steps):
        total = planes(i, total, i + 1 < steps)
    out[...] = total + z_pairs(z, zr)


def z_pairs(z, zr):
    gz = lax.axis_index("gz")
    at = lax.rem(lanes(), 4)
    parts = Total()
    for h in range(2):
        for v in range(TILES):
            own, other = z[h, v], zr[h, v]
            up = 2.0 * own - jnp.where(gz == 0, other, 0.0)
            down = jnp.where(gz == 0, 0.0, -other)
            up = jnp.where(at == 1, 16.0 * pltpu.roll(up, NZL - 1, 1), 0.0) - pltpu.roll(up, NZL - 2, 1)
            down = jnp.where(at == 2, 16.0 * pltpu.roll(down, 1, 1), 0.0) - pltpu.roll(down, 2, 1)
            parts.add(own * jnp.where(at < 2, up, down))
    return parts.value()


def first_kernel(load, stiff, b, dinv, kp, ex, ox, ey, oy, z, sums, raw, s, sem_b, sem_s):
    step = NXL // PARTS

    def copies(i):
        at = pl.ds(i * step, step)
        return (
            pltpu.make_async_copy(load.at[at], raw.at[at], sem_b.at[i]),
            pltpu.make_async_copy(stiff.at[at], s.at[at], sem_s.at[i]),
        )

    for i in range(PARTS):
        for c in copies(i):
            c.start()
    clear_sides(kp)

    def planes(i, carry):
        packed, total = carry
        for x in range(AT_ONCE):
            packed = finish_plane(kp, AT_ONCE * jnp.maximum(i - 1, 0) + x, packed)
        parts = Total()
        for x in [AT_ONCE * i + x for x in range(AT_ONCE)]:
            for v in range(TILES):
                row = pl.ds(v, 8, stride=TILES)
                inverse = 1.0 / (90.0 + 12.0 * s[x, row, :])
                right = 12.0 * raw[x, row, :]
                k = right * inverse
                b[x, v] = right
                dinv[x, v] = inverse
                kp[x + 2, v + 2] = k
                parts.add(k * right)
        return packed, total + parts.value()

    (total,) = zeros(1)
    packed = zeros(TILES)
    for i in range(PARTS):
        for c in copies(i):
            c.wait()
        packed, total = lax.fori_loop(i * step // AT_ONCE, (i + 1) * step // AT_ONCE, planes, (packed, total))
        if (i + 1) * step % 32 == 0:
            for x in range(AT_ONCE):
                packed = finish_plane(kp, (i + 1) * step - AT_ONCE + x, packed)
            for v in range(TILES):
                z[(i + 1) * step // 32 - 1, v] = packed[v]
    sums[0] = total
    send_faces(kp, ex, ox, ey, oy)


def across_kernel(
    first, part, kp, prev, dinv, exr, oxr, eyr, oyr, acc, kn, ex, ox, ey, oy, z, sums, rows, tiles
):
    del part
    gx, gy, _ = place()
    sub = lax.broadcasted_iota(jnp.int32, (8, NZL), 0)
    clear_sides(kn)
    for x, extra in zip((0, 1, NXL - 2, NXL - 1), over(*taken(exr[...], oxr[...], gx, 15))):
        acc[x] = acc[x] + extra
    for j, extra in enumerate(over(*taken(eyr[...], oyr[...], gy, 3))):
        rows[j] = extra
    for x in range(NXL):
        for j in range(4):
            tiles[x, j] = jnp.where(sub == (0 if j < 2 else 7), rows[j, x : x + 1, :], 0.0)

    packed = zeros(TILES)
    s0, s1 = zeros(2)
    for i in range(NXL // AT_ONCE + 1):
        for x in range(AT_ONCE if i else 0):
            packed = finish_plane(kn, AT_ONCE * (i - 1) + x, packed)
        if AT_ONCE * i in (NXL // 2, NXL):
            for v in range(TILES):
                z[AT_ONCE * i // (NXL // 2) - 1, v] = packed[v]
        if AT_ONCE * i == NXL:
            break
        p0, p1 = Total(), Total()
        for x in [AT_ONCE * i + x for x in range(AT_ONCE)]:
            for v in range(TILES):
                a = acc[x, v]
                if v in (0, 1, 6, 7):
                    a = a + tiles[x, v if v < 2 else v - 4]
                change = prev[x, v] - a
                new = change if first else a
                k = new * dinv[x, v]
                acc[x, v] = new
                kn[x + 2, v + 2] = k
                p0.add(kp[x + 2, v + 2] * change)
                p1.add(k * change)
        s0 = s0 + p0.value()
        s1 = s1 + p1.value()
    sums[0] = s0
    sums[1] = s1
    send_faces(kn, ex, ox, ey, oy)


def last_kernel(*refs):
    sums0, sums1, sums2, part = refs[:4]
    ex, ox, ey, oy, exr, oxr, eyr, oyr = refs[4:12]
    pairs = (refs[12:14], refs[14:16], (oy, oyr))
    row, own, sent = refs[16:]
    gx, gy, _ = place()
    m4 = part[...]
    for e, o, er, orr, at, last in ((ex, ox, exr, oxr, gx, 15), (ey, oy, eyr, oyr, gy, 3)):
        low, high = sides(e[...], o[...], at, last)
        extra = over(*taken(er[...], orr[...], at, last))
        gain = low[0] * extra[0] + low[1] * extra[1] + high[0] * extra[2] + high[1] * extra[3]
        m4 = m4 - gain.reshape(8, 8, NZL).sum(axis=0)
    parts = (sums0[0], sums1[0], sums1[1], sums2[0], sums2[1], m4)
    lane = lanes()
    sub = lax.broadcasted_iota(jnp.int32, (8, NZL), 0)
    stack = jnp.zeros((8, NZL), F32)
    for i, p in enumerate(parts):
        stack = jnp.where(sub == i, jnp.sum(p, axis=0, keepdims=True), stack)
    whole = jnp.sum(stack, axis=1, keepdims=True)
    out = jnp.sum(jnp.where(lane == sub, whole, 0.0), axis=0, keepdims=True)
    row[...] = jnp.broadcast_to(out, (128, NZL))
    below = gy == 1
    for j, (mine, other) in enumerate(pairs):
        mine, other = mine[...], other[...]
        a = jnp.where(below, mine, other)
        b = jnp.where(below, other, mine)
        t = (a[0] - b[1] + 27.0 * (b[0] - a[1])) * (1.0 / 24.0)
        sent[j] = jnp.where(below, t[0:16], t[48:64])
        own[j] = jnp.where(below, t[16:32], t[32:48])


def coefficients(rows):
    tot = jnp.sum(rows, axis=0, keepdims=True)
    lane = lax.broadcasted_iota(jnp.int32, (1, NZL), 1)
    v = [jnp.sum(jnp.where(lane == i, tot, 0.0), axis=1, keepdims=True) for i in range(6)]
    v0, g00, g01, g11, g12, g22 = v
    g02 = g01 - g11
    l1 = g01 / g00
    l2 = g02 / g00
    d1 = g11 - l1 * g01
    e = g12 - l2 * g01
    f1 = g00 - l1 * v0
    l3 = e / d1
    d2 = (g22 - l2 * g02) - l3 * e
    f2 = ((g00 - g01) - l2 * v0) - l3 * f1
    one = d1 > 3e-7 * g11
    two = jnp.logical_and(one, d2 > 3e-7 * g22)
    c2 = jnp.where(two, f2 / d2, 0.0)
    c1 = jnp.where(one, (f1 - e * c2) / d1, 0.0)
    c0 = (v0 - g01 * c1 - g02 * c2) / g00
    return c0, c1, c2


def scaled_sinh(a, s):
    half = 0.6931471805599453
    large = jnp.exp(a - s - half) - jnp.exp(-a - s - half)
    q = a * a
    small = a * (1.0 + q * (1.0 / 6.0 + q * (1.0 / 120.0 + q * (1.0 / 5040.0)))) * jnp.exp(-s)
    return jnp.where(jnp.abs(a) < 0.5, small, large)


def final_kernel(
    k0, k2, k1, rows, own, got, prestress, state, normal, out, slip, r0, r2, buf, sem0, sem2, sem
):
    gy = lax.axis_index("gy")
    step = NXL // PARTS

    def reads(i):
        at = pl.ds(2 + i * step, step)
        to = pl.ds(i * step, step)
        return (
            pltpu.make_async_copy(k0.at[at, pl.ds(2, TILES)], r0.at[to], sem0.at[i]),
            pltpu.make_async_copy(k2.at[at, pl.ds(2, TILES)], r2.at[to], sem2.at[i]),
        )

    def write(i):
        at = pl.ds(i * step, step)
        return pltpu.make_async_copy(buf.at[at], out.at[at], sem.at[i])

    for i in range(PARTS):
        for c in reads(i):
            c.start()
    c0, c1, c2 = coefficients(rows[...])

    def plane(x, carry):
        for v in range(TILES):
            at = pl.ds(v, 8, stride=TILES)
            buf[x, at, :] = c0 * r0[x, v] + c1 * k1[x + 2, v + 2] + c2 * r2[x, v]
        return carry

    for i in range(PARTS):
        for c in reads(i):
            c.wait()
        lax.fori_loop(i * step, (i + 1) * step, plane, 0)
        write(i).start()
    mine = jnp.logical_or(gy == 1, gy == 2)
    t = jnp.where(mine, own[...], got[...])
    traction = c0 * t[0] + c1 * t[1] + c2 * t[2]
    arg = (prestress[...] + 2.0 * traction) / normal[...]
    slip[...] = scaled_sinh(arg, state[...])
    for i in range(PARTS):
        write(i).wait()


def swap(x, axes, pairs):
    return lax.ppermute(x, axes, [*pairs, *((b, a) for a, b in pairs)])


def odd_pairs(along):
    pairs = []
    for gx in range(16):
        for gy in range(4):
            for gz in range(2):
                at, count = (gx, 16) if along == "gx" else (gy, 4)
                here = (gx * 4 + gy) * 2 + gz
                step = 8 if along == "gx" else 2
                if at % 2 == 1 and at < count - 1:
                    pairs.append((here, here + step))
                elif at in (0, count - 1) and gz == 0:
                    pairs.append((here, here + 1))
    return pairs


def exchange(ex, ox, ey, oy, z):
    evens = [(2 * i, 2 * i + 1) for i in range(8)]
    zr = swap(z, "gz", [(0, 1)])
    return (
        swap(ex, GX, evens),
        swap(ox, ALL, odd_pairs("gx")),
        swap(ey, "gy", [(0, 1), (2, 3)]),
        swap(oy, ALL, odd_pairs("gy")),
        zr,
    )


VM = pl.BlockSpec(memory_space=pltpu.VMEM)
HB = pl.BlockSpec(memory_space=pltpu.HBM)
BLOCK = (NXL, NYL, NZL)
TILED = (NXL, TILES, 8, NZL)
PADDED = (PX, TILES + 4, 8, NZL)
FACE = (2, TILES, 8, NZL)
FACES = (FACE, FACE, (2, NXL, NZL), (2, NXL, NZL), FACE)


def call(kernel, name, args, outs, scratch, aliases=None):
    return pl.pallas_call(
        kernel,
        out_shape=tuple(vmem(s) for s in outs),
        in_specs=[VM] * len(args),
        out_specs=(VM,) * len(outs),
        input_output_aliases=aliases or {},
        scratch_shapes=[vmem(s) for s in scratch],
        compiler_params=pltpu.CompilerParams(vmem_limit_bytes=LIMIT),
        cost_estimate=cost(),
        name=name,
    )(*map(in_vmem, args))


def cost():
    return pl.CostEstimate(flops=20_000_000, bytes_accessed=10_000_000, transcendentals=0)


def across(name, k, faces, prev, dinv):
    exr, oxr, eyr, oyr, zr = exchange(*faces)
    (part,) = call(inside_kernel, name + "_inside", (k, faces[-1], zr), (TILED,), (FACE, TILED, TILED, TILED))
    acc, kn, *rest = call(
        functools.partial(across_kernel, name == "one"),
        name + "_across",
        (part, k, prev, dinv, exr, oxr, eyr, oyr),
        (TILED, PADDED, *FACES, (2, 8, NZL)),
        ((4, NXL, NZL), (NXL, 4, 8, NZL)),
        {0: 0},
    )
    return acc, kn, rest[:-1], rest[-1], oyr


def per_device(load, stiffness, prestress, state_var, normal_a):
    outs = (TILED, TILED, PADDED, *FACES, (1, 8, NZL))
    b, dinv, k0, *faces, sums0 = pl.pallas_call(
        first_kernel,
        out_shape=tuple(vmem(s) for s in outs),
        in_specs=[HB, HB],
        out_specs=(VM,) * len(outs),
        scratch_shapes=[vmem(BLOCK), vmem(BLOCK), pltpu.SemaphoreType.DMA((PARTS,)), pltpu.SemaphoreType.DMA((PARTS,))],
        compiler_params=pltpu.CompilerParams(vmem_limit_bytes=LIMIT),
        cost_estimate=cost(),
        name="start",
    )(in_hbm(load), in_hbm(stiffness))
    e1, k1, faces1, sums1, oyr0 = across("one", k0, faces, b, dinv)
    e2, k2, faces2, sums2, oyr1 = across("two", k1, faces1, e1, dinv)
    taken2 = exchange(*faces2)
    (part,) = call(inside_sum_kernel, "three_inside", (k2, e2, faces2[4], taken2[4]), ((8, NZL),), (TILED,))
    row, own, sent = call(
        last_kernel,
        "last",
        (sums0, sums1, sums2, part, *faces2[:4], *taken2[:4], faces[3], oyr0, faces1[3], oyr1),
        ((128, NZL), (3, 16, NZL), (3, 16, NZL)),
        (),
    )
    got = swap(sent, "gy", [(0, 1), (2, 3)])
    rows = lax.all_to_all(row, ALL, 0, 0, tiled=True)
    out, slip = pl.pallas_call(
        final_kernel,
        out_shape=(jax.ShapeDtypeStruct(BLOCK, F32), jax.ShapeDtypeStruct((16, NZL), F32)),
        in_specs=[HB] * 2 + [VM] * 7,
        out_specs=(HB, VM),
        scratch_shapes=[vmem(TILED), vmem(TILED), vmem(BLOCK)] + [pltpu.SemaphoreType.DMA((PARTS,))] * 3,
        compiler_params=pltpu.CompilerParams(vmem_limit_bytes=LIMIT),
        cost_estimate=cost(),
        name="final",
    )(*map(in_hbm, (k0, k2)), *map(in_vmem, (k1, rows, own, got)), prestress, state_var, normal_a)
    return out, slip


def solution(mesh):
    torus = Mesh(
        mesh.devices.reshape(4, 4, mesh.shape["gy"], mesh.shape["gz"]), ("gx_0", "gx_1", "gy", "gz")
    )
    block = P(GX, "gy", "gz")
    fault = P(GX_GY, "gz")
    return jax.shard_map(
        per_device,
        mesh=torus,
        in_specs=(block, block, fault, fault, fault),
        out_specs=(block, fault),
        check_vma=False,
    )
```
